32 devices in a mesh: dp: 16 (over z, y, core), tensor: 2 (over x).
Axes of the slice: x: 2, y: 2, z: 4, core: 2. Of those that a mesh axis runs over, the one named last changes fastest.
Arguments:
- tokens: bfloat16 [32, 1024, 768], P(None, ('dp', 'tensor')), may hold values from -6 to 6
- out_grad: bfloat16 [32, 1024, 768], P(None, ('dp', 'tensor')), may hold values from -6 to 6
- lengths: int32 [32], replicated, may hold values from 256 to 1024, as said below
- order: int32 [1024], replicated, may hold values from 0 to 1023, each once
- w_qkv: bfloat16 [3, 768, 768], P(None, 'dp', 'tensor'), may hold values from -0.21875 to 0.21875
- b_qkv: float32 [3, 768], P(None, 'tensor'), may hold values from -3 to 3
- w_out: bfloat16 [768, 768], P('tensor', 'dp'), may hold values from -6 to 6
- b_out: float32 [768], replicated, may hold values from -3 to 3
- norm1_gain: float32 [768], replicated, may hold values from 0.25 to 1.75
- norm1_bias: float32 [768], replicated, may hold values from -2 to 2
- w_up: bfloat16 [768, 3072], P('dp', 'tensor'), may hold values from -0.21875 to 0.21875
- b_up: float32 [3072], P('tensor'), may hold values from -3 to 3
- w_down: bfloat16 [3072, 768], P('tensor', 'dp'), may hold values from -0.15625 to 0.15625
- b_down: float32 [768], replicated, may hold values from -3 to 3
- norm2_gain: float32 [768], replicated, may hold values from 0.25 to 1.75
- norm2_bias: float32 [768], replicated, may hold values from -2 to 2
Outputs:
- mixed: bfloat16 [32, 1024, 768], P(None, ('dp', 'tensor'))
- grad_tokens: bfloat16 [32, 1024, 768], P(None, ('dp', 'tensor'))
- grad_w_qkv: float32 [3, 768, 768], P(None, 'dp', 'tensor')
- grad_b_qkv: float32 [3, 768], replicated
- grad_w_out: float32 [768, 768], P('tensor', 'dp')
- grad_b_out: float32 [768], replicated
- grad_norm1_gain: float32 [768], replicated
- grad_norm1_bias: float32 [768], replicated
- grad_w_up: float32 [768, 3072], P('dp', 'tensor')
- grad_b_up: float32 [3072], replicated
- grad_w_down: float32 [3072, 768], P('tensor', 'dp')
- grad_b_down: float32 [768], replicated
- grad_norm2_gain: float32 [768], replicated
- grad_norm2_bias: float32 [768], replicated
The draws below stay inside these ranges and needn't reach their ends.
Inputs may be any that keep to these rules, and one draw needn't show every extreme that they name: `lengths`: one sequence in every draw has length 1024. `order`: the same for every sequence, each position once.
All inputs are finite; a program needn't handle non-finite values.
Results may differ from the reference program's by a relative error of at most 0.019.
Values may be sent and summed in bfloat16 or wider, within the bound.
A program may use at most 192 MiB of HBM per device.

```python
import jax
import jax.numpy as jnp
from jax import lax

D = 768
H = 12
HD = 64
FF = 3072
SLOT = 1024
MIN_LEN = 256
NSEQ = 32


def draw_lengths(key, part):
    first_key, second_key = jax.random.split(jax.random.fold_in(key, 11))
    drawn = jax.random.randint(first_key, (NSEQ,), MIN_LEN, SLOT + 1)
    chosen = jax.random.randint(second_key, (), 0, NSEQ)
    return jnp.where(jnp.arange(NSEQ) == chosen, SLOT, drawn).astype(jnp.int32)


def levels(key, extent, cuts, least, largest):
    def one(dim, parts):
        draws = jax.random.uniform(jax.random.fold_in(jax.random.fold_in(key, 6), dim), (parts,), jnp.float32, least / len(cuts), largest / len(cuts))
        return jnp.repeat(jnp.exp(draws), extent[dim] // parts).reshape((-1,) + (1,) * (len(extent) - dim - 1))

    loudness = one(*cuts[0])
    for cut in cuts[1:]:
        loudness = loudness * one(*cut)
    return loudness


def gaussian(rng, shape, scale, most, pieces=(), held_as=jnp.bfloat16):
    entries = scale * jax.random.normal(rng, shape, jnp.float32)
    if pieces:
        entries = entries * levels(rng, shape, pieces, -0.22, 0.18)
    return jnp.clip(entries, -most, most).astype(held_as)


def setup_inputs(seed: int = 0) -> dict:
    splits = jax.random.split(jax.random.key(seed), 17)
    return {
        "tokens": gaussian(splits[0], (NSEQ, SLOT, D), 1.0, 6.0, ((1, 32),)),
        "out_grad": gaussian(splits[1], (NSEQ, SLOT, D), 1.0, 6.0, ((1, 32),)),
        "lengths": draw_lengths(jax.random.fold_in(splits[16], 71), 0),
        "order": jax.random.permutation(splits[3], SLOT).astype(jnp.int32),
        "w_qkv": gaussian(splits[4], (3, D, D), D ** -0.5, 0.21875, ((1, 16), (2, 2))),
        "b_qkv": gaussian(splits[5], (3, D), 0.5, 3.0, ((1, 2),), jnp.float32),
        "w_out": gaussian(splits[6], (D, D), (max(1, D * 2 // SLOT)) ** -0.5, 6.0, ((0, 2), (1, 16))),
        "b_out": gaussian(splits[7], (D,), 0.5, 3.0, (), jnp.float32),
        "norm1_gain": jnp.clip(1.0 + 0.15 * jax.random.normal(splits[8], (D,), jnp.float32), 0.25, 1.75),
        "norm1_bias": gaussian(splits[9], (D,), 0.3, 2.0, (), jnp.float32),
        "w_up": gaussian(splits[10], (D, FF), D ** -0.5, 0.21875, ((0, 16), (1, 2))),
        "b_up": gaussian(splits[11], (FF,), 0.5, 3.0, ((0, 2),), jnp.float32),
        "w_down": gaussian(splits[12], (FF, D), (FF // 2) ** -0.5, 0.15625, ((0, 2), (1, 16))),
        "b_down": gaussian(splits[13], (D,), 0.5, 3.0, (), jnp.float32),
        "norm2_gain": jnp.clip(1.0 + 0.15 * jax.random.normal(splits[14], (D,), jnp.float32), 0.25, 1.75),
        "norm2_bias": gaussian(splits[15], (D,), 0.3, 2.0, (), jnp.float32),
    }


NORM_EPS = 1e-12
ROPE_BASE = 10000.0
MASK_FILL = -1e+30
SCORE_SCALE = 0.125

@jax.custom_vjp
def low(v):
    return lax.optimization_barrier(v.astype(jnp.bfloat16)).astype(jnp.float32)

@jax.custom_vjp
def low_back(v):
    return v

def low_keep(v):
    return (low(v), None)

def low_pass(kept, grad):
    return (grad,)

def back_keep(v):
    return (v, None)

def back_low(kept, grad):
    return (low(grad),)
low.defvjp(low_keep, low_pass)
low_back.defvjp(back_keep, back_low)

def rope_tables(positions):
    steps = jnp.arange(HD // 2).astype(jnp.float32)
    inverse = jnp.power(ROPE_BASE, -2.0 * steps / HD)
    angles = positions.astype(jnp.float32)[:, None] * inverse[None, :]
    return (jnp.cos(angles), jnp.sin(angles))

def rotate(values, cos_table, sine_table):
    shaped = values.reshape(values.shape[0], values.shape[1], values.shape[2] // 2, 2)
    first = shaped[..., 0]
    second = shaped[..., 1]
    cos_part = cos_table[:, None, :]
    sine_part = sine_table[:, None, :]
    turned = jnp.stack([first * cos_part - second * sine_part, first * sine_part + second * cos_part], axis=-1)
    return turned.reshape(values.shape)

def layer_norm(hidden, gain_vec, shift_vec):
    row_mean = lax.optimization_barrier(jnp.mean(hidden, axis=-1, keepdims=True))
    centred = hidden - row_mean
    row_var = lax.optimization_barrier(jnp.mean(centred * centred, axis=-1, keepdims=True))
    return centred * lax.rsqrt(row_var + NORM_EPS) * gain_vec + shift_vec

def one_sequence(sequence, positions, length, cos_table, sine_table, params):
    w_qkv, b_qkv, w_out, b_out, gain_one, shift_one, w_up, b_up, w_down, b_down, gain_two, shift_two = params
    highest = lax.Precision.HIGHEST
    raw_proj = low_back(jnp.einsum('sd,kde->kse', low(sequence), w_qkv, precision=highest) + b_qkv[:, None, :])
    query = low(rotate(raw_proj[0].reshape(SLOT, H, HD), cos_table, sine_table))
    keys_rot = low(rotate(raw_proj[1].reshape(SLOT, H, HD), cos_table, sine_table))
    value = low(raw_proj[2].reshape(SLOT, H, HD))
    scores = low_back(jnp.einsum('qhe,khe->hqk', query, keys_rot, precision=highest) * SCORE_SCALE)
    key_keep = positions < length
    scores = jnp.where(key_keep[None, None, :], scores, MASK_FILL)
    row_max = lax.optimization_barrier(jnp.max(scores, axis=-1, keepdims=True))
    expo_vals = jnp.exp(scores - row_max)
    prob_vals = expo_vals / lax.optimization_barrier(jnp.sum(expo_vals, axis=-1, keepdims=True))
    context = jnp.einsum('hqk,khe->qhe', low(prob_vals), value, precision=highest).reshape(SLOT, D)
    context = low_back(low(context))
    attended = low_back(jnp.dot(context, w_out, precision=highest))
    first_sum = sequence + attended + b_out
    normed_one = layer_norm(first_sum, gain_one, shift_one)
    up_proj = low_back(jnp.dot(low(normed_one), w_up, precision=highest) + b_up)
    activated = low(jax.nn.gelu(up_proj, approximate=False))
    down_proj = low_back(jnp.dot(activated, w_down, precision=highest))
    second_sum = normed_one + down_proj + b_down
    return layer_norm(second_sum, gain_two, shift_two)

def reference(tokens, out_grad, lengths, order, w_qkv, b_qkv, w_out, b_out, norm1_gain, norm1_bias, w_up, b_up, w_down, b_down, norm2_gain, norm2_bias):
    cos_table, sine_table = rope_tables(order)
    params = (w_qkv.astype(jnp.float32), b_qkv.astype(jnp.float32), w_out.astype(jnp.float32), b_out.astype(jnp.float32), norm1_gain.astype(jnp.float32), norm1_bias.astype(jnp.float32), w_up.astype(jnp.float32), b_up.astype(jnp.float32), w_down.astype(jnp.float32), b_down.astype(jnp.float32), norm2_gain.astype(jnp.float32), norm2_bias.astype(jnp.float32))

    def forward(inputs, weights):

        def scan_step(carry_val, pair_item):
            sequence, length = pair_item
            return (carry_val, one_sequence(sequence, order, length, cos_table, sine_table, weights))
        unused, outputs = lax.scan(jax.checkpoint(scan_step), jnp.zeros((), jnp.float32), (inputs, lengths))
        return outputs
    mixed, pullback = jax.vjp(forward, tokens.astype(jnp.float32), params)
    keep_rows = order[None, :] < lengths[:, None]
    cotangent = jnp.where(keep_rows[:, :, None], out_grad.astype(jnp.float32), 0.0)
    grad_in, grad_params = pullback(cotangent)
    return (mixed.astype(jnp.bfloat16), grad_in.astype(jnp.bfloat16), grad_params[0], grad_params[1], grad_params[2], grad_params[3], grad_params[4], grad_params[5], grad_params[6], grad_params[7], grad_params[8], grad_params[9], grad_params[10], grad_params[11])
```

```python
import functools

import jax
import jax.numpy as jnp
from jax import lax
from jax.experimental import pallas as pl
from jax.experimental.pallas import tpu as pltpu
from jax.sharding import PartitionSpec as P

HD = 64
LANES = 128
NORM_EPS = 1e-12
ROPE_BASE = 10000.0
MASK_FILL = -1e30
SCORE_SCALE = 0.125
INV_ROOT_TWO = 0.7071067811865476
INV_ROOT_TAU = 0.3989422804014327
AXES = ("dp", "tensor")
BF = jnp.bfloat16
F32 = jnp.float32
VMEM_BYTES = 60 * 1024 * 1024


def dot(a, b, dims):
    return lax.dot_general(a, b, (dims, ((), ())), preferred_element_type=F32)


NN = ((1,), (0,))
NT = ((1,), (1,))
TN = ((0,), (0,))


def rope_tables(positions):
    steps = (jnp.arange(LANES) % HD // 2).astype(F32)
    inverse = jnp.power(ROPE_BASE, -2.0 * steps / HD)
    angles = positions.astype(F32)[:, None] * inverse[None, :]
    return jnp.cos(angles), jnp.sin(angles)


def turn(values, cos_table, sine_table):
    lane = lax.broadcasted_iota(jnp.int32, values.shape, 1)
    swapped = jnp.where(
        lane % 2 == 0, -pltpu.roll(values, LANES - 1, 1), pltpu.roll(values, 1, 1)
    )
    return values * cos_table + swapped * sine_table


def project_kernel(x_ref, w_ref, b_ref, cos_ref, sine_ref, out_ref):
    kind = pl.program_id(0)
    raw = dot(x_ref[...], w_ref[0], NN) + b_ref[0]

    @pl.when(kind < 2)
    def _():
        for part in range(raw.shape[1] // LANES):
            cols = slice(part * LANES, (part + 1) * LANES)
            out_ref[0, :, cols] = turn(raw[:, cols], cos_ref[...], sine_ref[...]).astype(BF)

    @pl.when(kind == 2)
    def _():
        out_ref[0] = raw.astype(BF)


def project(x, w, b, cos_table, sine_table):
    rows, features = x.shape
    block = 256
    return pl.pallas_call(
        project_kernel,
        grid=(3, features // block),
        in_specs=[
            pl.BlockSpec((rows, features), lambda p, c: (0, 0)),
            pl.BlockSpec((1, features, block), lambda p, c: (p, 0, c)),
            pl.BlockSpec((1, 1, block), lambda p, c: (p, 0, c)),
            pl.BlockSpec((rows, LANES), lambda p, c: (0, 0)),
            pl.BlockSpec((rows, LANES), lambda p, c: (0, 0)),
        ],
        out_specs=pl.BlockSpec((1, rows, block), lambda p, c: (p, 0, c)),
        out_shape=jax.ShapeDtypeStruct((3, rows, features), BF),
        compiler_params=pltpu.CompilerParams(vmem_limit_bytes=VMEM_BYTES),
        name="project",
    )(x, w, b, cos_table, sine_table)


def head_masks(rows):
    lane = lax.broadcasted_iota(jnp.int32, (rows, LANES), 1)
    return lane


def pair_operands(q, k, bias, lane, head):
    inside = lane // HD == head
    spare = lane == (1 - head) * HD
    zero = jnp.zeros_like(q)
    q_head = jnp.where(inside, q, jnp.where(spare, jnp.ones_like(q), zero))
    k_head = jnp.where(inside, k, jnp.where(spare, bias, zero))
    return q_head, k_head


def attend_kernel(q_ref, k_ref, v_ref, bias_ref, ctx_ref, lse_ref, *, chunk):
    rows = q_ref.shape[1]
    lane = lax.broadcasted_iota(jnp.int32, (rows, LANES), 1)
    q = q_ref[0] * jnp.asarray(SCORE_SCALE, BF)
    k = k_ref[0]
    v_turned = v_ref[0].T
    bias = bias_ref[...]
    for part in range(rows // chunk):
        span = slice(part * chunk, (part + 1) * chunk)
        outs = []
        for head in range(2):
            q_head, k_head = pair_operands(q, k, bias, lane, head)
            scores = dot(k_head, q_head[span], NT)
            top = jnp.max(scores, axis=0, keepdims=True)
            expo = jnp.exp(scores - top)
            total = jnp.sum(expo, axis=0, keepdims=True)
            mixed = dot(v_turned[head * HD : (head + 1) * HD], expo.astype(BF), NN)
            outs.append(mixed / total)
            lse_ref[0, head : head + 1, span] = top + jnp.log(total)
        ctx_ref[span, :] = jnp.concatenate(outs, axis=0).T.astype(BF)


def attend(qkv, bias):
    _, rows, features = qkv.shape
    pairs = features // LANES
    chunk = 256

    def spec(which):
        return pl.BlockSpec((1, rows, LANES), lambda h: (which, 0, h))

    return pl.pallas_call(
        functools.partial(attend_kernel, chunk=chunk),
        grid=(pairs,),
        in_specs=[spec(0), spec(1), spec(2), pl.BlockSpec((rows, LANES), lambda h: (0, 0))],
        out_specs=[
            pl.BlockSpec((rows, LANES), lambda h: (0, h)),
            pl.BlockSpec((1, 2, rows), lambda h: (h, 0, 0)),
        ],
        out_shape=[
            jax.ShapeDtypeStruct((rows, features), BF),
            jax.ShapeDtypeStruct((pairs, 2, rows), F32),
        ],
        compiler_params=pltpu.CompilerParams(vmem_limit_bytes=VMEM_BYTES),
        name="attend",
    )(qkv, qkv, qkv, bias)


def attend_back_kernel(
    q_ref, k_ref, v_ref, bias_ref, ctx_ref, grad_ref, lse_ref, cos_ref, sine_ref, out_ref,
    dk_ref, dv_ref, *, chunk
):
    rows = q_ref.shape[1]
    lane = lax.broadcasted_iota(jnp.int32, (rows, LANES), 1)
    q = q_ref[0] * jnp.asarray(SCORE_SCALE, BF)
    k = k_ref[0]
    v = v_ref[0]
    grad = grad_ref[...]
    bias = bias_ref[...]
    k_turned = k.T
    zero = jnp.zeros_like(grad)
    dots = (grad.astype(F32) * ctx_ref[...].astype(F32)).T
    for part in range(rows // chunk):
        span = slice(part * chunk, (part + 1) * chunk)
        dq_parts = []
        dk_sum = None
        dv_sum = None
        for head in range(2):
            q_head, k_head = pair_operands(q, k, bias, lane, head)
            inside = lane // HD == head
            g_head = jnp.where(inside, grad, zero)[span]
            q_only = jnp.where(inside, q, zero)[span]
            scores = dot(k_head, q_head[span], NT)
            prob = jnp.exp(scores - lse_ref[0, head : head + 1, span])
            g_prob = dot(v, g_head, NT)
            inner = jnp.sum(dots[head * HD : (head + 1) * HD, span], axis=0, keepdims=True)
            g_score = (prob * (g_prob - inner)).astype(BF)
            dv = dot(prob.astype(BF), g_head, NN)
            dk = dot(g_score, q_only, NN)
            dq_parts.append(dot(k_turned[head * HD : (head + 1) * HD], g_score, NN))
            dk_sum = dk if dk_sum is None else dk_sum + dk
            dv_sum = dv if dv_sum is None else dv_sum + dv
        dq = jnp.concatenate(dq_parts, axis=0).T * SCORE_SCALE
        out_ref[0, span, :] = turn(dq, cos_ref[span, :], -sine_ref[span, :]).astype(BF)
        if part == 0:
            dk_ref[...] = dk_sum
            dv_ref[...] = dv_sum
        else:
            dk_ref[...] += dk_sum
            dv_ref[...] += dv_sum
    out_ref[1] = turn(dk_ref[...], cos_ref[...], -sine_ref[...]).astype(BF)
    out_ref[2] = dv_ref[...].astype(BF)


def attend_back(qkv, bias, context, grad_ctx, lse, cos_table, sine_table):
    _, rows, features = qkv.shape
    pairs = features // LANES
    chunk = 256

    def spec(which):
        return pl.BlockSpec((1, rows, LANES), lambda h: (which, 0, h))

    fixed = pl.BlockSpec((rows, LANES), lambda h: (0, 0))
    cols = pl.BlockSpec((rows, LANES), lambda h: (0, h))
    return pl.pallas_call(
        functools.partial(attend_back_kernel, chunk=chunk),
        grid=(pairs,),
        in_specs=[
            spec(0), spec(1), spec(2), fixed, cols, cols,
            pl.BlockSpec((1, 2, rows), lambda h: (h, 0, 0)), fixed, fixed,
        ],
        out_specs=pl.BlockSpec((3, rows, LANES), lambda h: (0, 0, h)),
        out_shape=jax.ShapeDtypeStruct((3, rows, features), BF),
        scratch_shapes=[pltpu.VMEM((rows, LANES), F32), pltpu.VMEM((rows, LANES), F32)],
        compiler_params=pltpu.CompilerParams(vmem_limit_bytes=VMEM_BYTES),
        name="attend_back",
    )(qkv, qkv, qkv, bias, context, grad_ctx, lse, cos_table, sine_table)


def normalize(hidden, gain_vec, shift_vec):
    row_mean = jnp.mean(hidden, axis=-1, keepdims=True)
    centred = hidden - row_mean
    row_var = jnp.mean(centred * centred, axis=-1, keepdims=True)
    inv_std = lax.rsqrt(row_var + NORM_EPS)
    normed = centred * inv_std
    return (normed * gain_vec + shift_vec, normed, inv_std)


def normalize_back(grad_unit, normed, inv_std):
    first_mean = jnp.mean(grad_unit, axis=-1, keepdims=True)
    second_mean = jnp.mean(grad_unit * normed, axis=-1, keepdims=True)
    return inv_std * (grad_unit - first_mean - normed * second_mean)


def gelu_slope(up_proj):
    return (
        0.5 * (1.0 + lax.erf(up_proj * INV_ROOT_TWO))
        + up_proj * jnp.exp(-0.5 * up_proj * up_proj) * INV_ROOT_TAU
    )


def layer(rows, cotangent, place, length, cos_table, sine_table, params):
    (w_qkv, b_qkv, w_out_t, b_out, gain_one, shift_one, w_up, b_up, w_down_t, b_down,
     gain_two, shift_two) = params
    live = place < length
    bias = jnp.broadcast_to(jnp.where(live, 0.0, MASK_FILL).astype(BF)[:, None], (rows.shape[0], LANES))
    qkv = project(rows, w_qkv, b_qkv[:, None, :], cos_table, sine_table)
    context, lse = attend(qkv, bias)
    first_sum = rows.astype(F32) + dot(context, w_out_t, NT) + b_out
    normed_one, unit_one, inv_one = normalize(first_sum, gain_one, shift_one)
    mid = normed_one.astype(BF)
    up_proj = dot(mid, w_up, NN) + b_up
    activated = jax.nn.gelu(up_proj, approximate=False).astype(BF)
    second_sum = normed_one + dot(activated, w_down_t, NT) + b_down
    result, unit_two, inv_two = normalize(second_sum, gain_two, shift_two)
    result = result.astype(BF)

    grad_out = jnp.where(live[:, None], cotangent.astype(F32), 0.0)
    g_gain_two = jnp.sum(grad_out * unit_two, axis=0)
    g_shift_two = jnp.sum(grad_out, axis=0)
    grad_second = normalize_back(grad_out * gain_two, unit_two, inv_two)
    g_b_down = jnp.sum(grad_second, axis=0)
    grad_down = grad_second.astype(BF)
    g_w_down_t = dot(grad_down, activated, TN)
    grad_up = (dot(grad_down, w_down_t, NN) * gelu_slope(up_proj)).astype(BF)
    g_b_up = jnp.sum(grad_up.astype(F32), axis=0)
    g_w_up = dot(mid, grad_up, TN)
    grad_mid = grad_second + dot(grad_up, w_up, NT)
    g_gain_one = jnp.sum(grad_mid * unit_one, axis=0)
    g_shift_one = jnp.sum(grad_mid, axis=0)
    grad_first = normalize_back(grad_mid * gain_one, unit_one, inv_one)
    g_b_out = jnp.sum(grad_first, axis=0)
    grad_attn = grad_first.astype(BF)
    g_w_out_t = dot(grad_attn, context, TN)
    grad_ctx = dot(grad_attn, w_out_t, NN).astype(BF)
    grad_raw = attend_back(qkv, bias, context, grad_ctx, lse, cos_table, sine_table)
    g_b_qkv = jnp.sum(grad_raw.astype(F32), axis=1)
    g_w_qkv = [dot(rows, grad_raw[i], TN) for i in range(3)]
    in_sum = sum(dot(grad_raw[i], w_qkv[i], NT) for i in range(3))
    grad_rows = (grad_first + in_sum).astype(BF)
    weights = (g_w_qkv, g_w_out_t, g_w_up, g_w_down_t)
    small = (g_b_qkv, g_b_out, g_gain_one, g_shift_one, g_b_up, g_b_down, g_gain_two, g_shift_two)
    return result, grad_rows, weights, small


def body(
    tokens, out_grad, lengths, order, w_qkv, b_qkv, w_out, b_out, norm1_gain, norm1_bias,
    w_up, b_up, w_down, b_down, norm2_gain, norm2_bias,
):
    dp_size = lax.axis_size("dp")
    tp_size = lax.axis_size("tensor")
    devices = dp_size * tp_size
    me = lax.axis_index(AXES)
    stored, stripe, features = tokens.shape
    batches = stored // devices
    slot = devices * stripe
    depth = w_qkv.shape[1]
    cols = w_qkv.shape[2]
    units = w_up.shape[1]

    def deal(rows_val):
        return lax.all_to_all(
            rows_val.reshape(batches, devices, stripe, features), AXES,
            split_axis=1, concat_axis=2, tiled=True,
        ).reshape(batches, slot, features)

    def give_back(rows_val):
        return lax.all_to_all(
            rows_val.reshape(batches, 1, slot, features), AXES,
            split_axis=2, concat_axis=1, tiled=True,
        ).reshape(stored, stripe, features)

    inputs = deal(tokens)
    attn_shard = jnp.concatenate([w_qkv.reshape(3 * depth, cols), w_out.T], axis=0)
    attn_all = lax.all_gather(attn_shard, AXES, axis=0, tiled=False)
    attn_all = attn_all.reshape(dp_size, tp_size, 4, depth, cols)
    attn_all = attn_all.transpose(2, 0, 3, 1, 4).reshape(4, features, features)
    ffn_shard = jnp.stack([w_up, w_down.T], axis=0)
    ffn_all = lax.all_gather(ffn_shard, AXES, axis=0, tiled=False)
    ffn_all = ffn_all.reshape(dp_size, tp_size, 2, depth, units)
    ffn_all = ffn_all.transpose(2, 0, 3, 1, 4).reshape(2, features, tp_size * units)
    b_qkv_all = lax.all_gather(b_qkv, "tensor", axis=1, tiled=True)
    b_up_all = lax.all_gather(b_up, "tensor", axis=0, tiled=True)
    cotangents = deal(out_grad)
    cos_table, sine_table = rope_tables(order)
    params = (attn_all[:3], b_qkv_all, attn_all[3], b_out, norm1_gain, norm1_bias,
              ffn_all[0], b_up_all, ffn_all[1], b_down, norm2_gain, norm2_bias)
    results, input_grads, weights, small = [], [], None, None
    for micro in range(batches):
        length = lax.dynamic_index_in_dim(lengths, micro * devices + me, 0, keepdims=False)
        result, grad_rows, weights_one, small_one = layer(
            inputs[micro], cotangents[micro], order, length, cos_table, sine_table, params
        )
        results.append(result)
        input_grads.append(grad_rows)
        if weights is None:
            weights, small = weights_one, small_one
        else:
            weights, small = jax.tree.map(jnp.add, (weights, small), (weights_one, small_one))
    mixed = give_back(jnp.stack(results, axis=0))
    grad_tokens = give_back(jnp.stack(input_grads, axis=0))

    def scatter(parts):
        laid = [
            p.astype(BF).reshape(dp_size, depth, tp_size, -1).transpose(0, 2, 1, 3) for p in parts
        ]
        laid = jnp.stack(laid, axis=2).reshape(devices, len(parts), depth, -1)
        return lax.psum_scatter(laid, AXES, scatter_dimension=0, tiled=False).astype(F32)

    g_qkv, g_out_t, g_up, g_down_t = weights
    ffn_sum = scatter([g_up, g_down_t])
    attn_sum = scatter(list(g_qkv) + [g_out_t])
    sizes = [s.size for s in small]
    packed = jnp.concatenate([s.reshape(-1) for s in small]).reshape(-1, LANES)
    summed = jnp.sum(lax.all_gather(packed, AXES, axis=0, tiled=False), axis=0).reshape(-1)
    small_sums, start = [], 0
    for s, size in zip(small, sizes):
        small_sums.append(summed[start : start + size].reshape(s.shape))
        start += size
    return (
        mixed, grad_tokens, attn_sum[:3], small_sums[0], attn_sum[3].T, small_sums[1],
        small_sums[2], small_sums[3], ffn_sum[0], small_sums[4], ffn_sum[1].T, small_sums[5],
        small_sums[6], small_sums[7],
    )


def solution(mesh):
    rows = P(None, AXES, None)
    in_specs = (
        rows, rows, P(), P(), P(None, "dp", "tensor"), P(None, "tensor"), P("tensor", "dp"), P(),
        P(), P(), P("dp", "tensor"), P("tensor"), P("tensor", "dp"), P(), P(), P(),
    )
    out_specs = (
        rows, rows, P(None, "dp", "tensor"), P(), P("tensor", "dp"), P(), P(), P(),
        P("dp", "tensor"), P(), P("tensor", "dp"), P(), P(), P(),
    )
    return jax.shard_map(body, mesh=mesh, in_specs=in_specs, out_specs=out_specs, check_vma=False)
```

```python
import functools

import jax
import jax.numpy as jnp
from jax import lax
from jax.experimental import pallas as pl
from jax.experimental.pallas import tpu as pltpu
from jax.sharding import PartitionSpec as P

HD = 64
LANES = 128
NORM_EPS = 1e-12
ROPE_BASE = 10000.0
MASK_FILL = -1e30
SCORE_SCALE = 0.125
INV_ROOT_TWO = 0.7071067811865476
INV_ROOT_TAU = 0.3989422804014327
AXES = ("dp", "tensor")
BF = jnp.bfloat16
F32 = jnp.float32
VMEM_BYTES = 60 * 1024 * 1024


def dot(a, b, dims):
    return lax.dot_general(a, b, (dims, ((), ())), preferred_element_type=F32)


NN = ((1,), (0,))
NT = ((1,), (1,))
TN = ((0,), (0,))


def rope_tables(positions):
    steps = (jnp.arange(LANES) % HD // 2).astype(F32)
    inverse = jnp.power(ROPE_BASE, -2.0 * steps / HD)
    angles = positions.astype(F32)[:, None] * inverse[None, :]
    return jnp.cos(angles), jnp.sin(angles)


def turn(values, cos_table, sine_table):
    lane = lax.broadcasted_iota(jnp.int32, values.shape, 1)
    swapped = jnp.where(
        lane % 2 == 0, -pltpu.roll(values, LANES - 1, 1), pltpu.roll(values, 1, 1)
    )
    return values * cos_table + swapped * sine_table


def block_rows(w_ref, member, part, depth, cols=slice(None)):
    taken = w_ref[:, member, part * depth : (part + 1) * depth, cols]
    return taken.reshape(taken.shape[0] * depth, taken.shape[2])


def project_kernel(x_ref, w_ref, b_ref, cos_ref, sine_ref, out_ref):
    kind = pl.program_id(0)
    depth = w_ref.shape[2]
    raw = dot(x_ref[...], block_rows(w_ref, 0, 0, depth), NN) + b_ref[0]

    @pl.when(kind < 2)
    def _():
        for part in range(raw.shape[1] // LANES):
            cols = slice(part * LANES, (part + 1) * LANES)
            out_ref[0, :, cols] = turn(raw[:, cols], cos_ref[...], sine_ref[...]).astype(BF)

    @pl.when(kind == 2)
    def _():
        out_ref[0] = raw.astype(BF)


def project(x, attn_w, b, cos_table, sine_table):
    rows, features = x.shape
    groups, members, depth4, cols = attn_w.shape
    depth = depth4 // 4
    return pl.pallas_call(
        project_kernel,
        grid=(3, members),
        in_specs=[
            pl.BlockSpec((rows, features), lambda p, c: (0, 0)),
            pl.BlockSpec((groups, 1, depth, cols), lambda p, c: (0, c, p, 0)),
            pl.BlockSpec((1, 1, cols), lambda p, c: (p, 0, c)),
            pl.BlockSpec((rows, LANES), lambda p, c: (0, 0)),
            pl.BlockSpec((rows, LANES), lambda p, c: (0, 0)),
        ],
        out_specs=pl.BlockSpec((1, rows, cols), lambda p, c: (p, 0, c)),
        out_shape=jax.ShapeDtypeStruct((3, rows, features), BF),
        compiler_params=pltpu.CompilerParams(vmem_limit_bytes=VMEM_BYTES),
        name="project",
    )(x, attn_w, b, cos_table, sine_table)


def pair_operands(q, k, bias, lane, head):
    inside = lane // HD == head
    spare = lane == (1 - head) * HD
    zero = jnp.zeros_like(q)
    q_head = jnp.where(inside, q, jnp.where(spare, jnp.ones_like(q), zero))
    k_head = jnp.where(inside, k, jnp.where(spare, bias, zero))
    return q_head, k_head


def attend_kernel(q_ref, k_ref, v_ref, bias_ref, ctx_ref, lse_ref, *, chunk):
    rows = q_ref.shape[1]
    lane = lax.broadcasted_iota(jnp.int32, (rows, LANES), 1)
    q = q_ref[0] * jnp.asarray(SCORE_SCALE, BF)
    k = k_ref[0]
    v_turned = v_ref[0].T
    bias = bias_ref[...]
    for part in range(rows // chunk):
        span = slice(part * chunk, (part + 1) * chunk)
        outs = []
        for head in range(2):
            q_head, k_head = pair_operands(q, k, bias, lane, head)
            scores = dot(k_head, q_head[span], NT)
            top = jnp.max(scores, axis=0, keepdims=True)
            expo = jnp.exp(scores - top)
            total = jnp.sum(expo, axis=0, keepdims=True)
            mixed = dot(v_turned[head * HD : (head + 1) * HD], expo.astype(BF), NN)
            outs.append(mixed / total)
            lse_ref[0, head : head + 1, span] = top + jnp.log(total)
        ctx_ref[span, :] = jnp.concatenate(outs, axis=0).T.astype(BF)


def attend(qkv, bias):
    _, rows, features = qkv.shape
    pairs = features // LANES
    chunk = 256

    def spec(which):
        return pl.BlockSpec((1, rows, LANES), lambda h: (which, 0, h))

    return pl.pallas_call(
        functools.partial(attend_kernel, chunk=chunk),
        grid=(pairs,),
        in_specs=[spec(0), spec(1), spec(2), pl.BlockSpec((rows, LANES), lambda h: (0, 0))],
        out_specs=[
            pl.BlockSpec((rows, LANES), lambda h: (0, h)),
            pl.BlockSpec((1, 2, rows), lambda h: (h, 0, 0)),
        ],
        out_shape=[
            jax.ShapeDtypeStruct((rows, features), BF),
            jax.ShapeDtypeStruct((pairs, 2, rows), F32),
        ],
        compiler_params=pltpu.CompilerParams(vmem_limit_bytes=VMEM_BYTES),
        name="attend",
    )(qkv, qkv, qkv, bias)


def attend_back_kernel(
    q_ref, k_ref, v_ref, bias_ref, ctx_ref, grad_ref, lse_ref, cos_ref, sine_ref, out_ref,
    dk_ref, dv_ref, *, chunk
):
    rows = q_ref.shape[1]
    lane = lax.broadcasted_iota(jnp.int32, (rows, LANES), 1)
    q = q_ref[0] * jnp.asarray(SCORE_SCALE, BF)
    k = k_ref[0]
    v = v_ref[0]
    grad = grad_ref[...]
    bias = bias_ref[...]
    k_turned = k.T
    zero = jnp.zeros_like(grad)
    dots = (grad.astype(F32) * ctx_ref[...].astype(F32)).T
    for part in range(rows // chunk):
        span = slice(part * chunk, (part + 1) * chunk)
        dq_parts = []
        dk_sum = None
        dv_sum = None
        for head in range(2):
            q_head, k_head = pair_operands(q, k, bias, lane, head)
            inside = lane // HD == head
            g_head = jnp.where(inside, grad, zero)[span]
            q_only = jnp.where(inside, q, zero)[span]
            scores = dot(k_head, q_head[span], NT)
            prob = jnp.exp(scores - lse_ref[0, head : head + 1, span])
            g_prob = dot(v, g_head, NT)
            inner = jnp.sum(dots[head * HD : (head + 1) * HD, span], axis=0, keepdims=True)
            g_score = (prob * (g_prob - inner)).astype(BF)
            dv = dot(prob.astype(BF), g_head, NN)
            dk = dot(g_score, q_only, NN)
            dq_parts.append(dot(k_turned[head * HD : (head + 1) * HD], g_score, NN))
            dk_sum = dk if dk_sum is None else dk_sum + dk
            dv_sum = dv if dv_sum is None else dv_sum + dv
        dq = jnp.concatenate(dq_parts, axis=0).T * SCORE_SCALE
        out_ref[0, span, :] = turn(dq, cos_ref[span, :], -sine_ref[span, :]).astype(BF)
        if part == 0:
            dk_ref[...] = dk_sum
            dv_ref[...] = dv_sum
        else:
            dk_ref[...] += dk_sum
            dv_ref[...] += dv_sum
    out_ref[1] = turn(dk_ref[...], cos_ref[...], -sine_ref[...]).astype(BF)
    out_ref[2] = dv_ref[...].astype(BF)


def attend_back(qkv, bias, context, grad_ctx, lse, cos_table, sine_table):
    _, rows, features = qkv.shape
    pairs = features // LANES
    chunk = 256

    def spec(which):
        return pl.BlockSpec((1, rows, LANES), lambda h: (which, 0, h))

    fixed = pl.BlockSpec((rows, LANES), lambda h: (0, 0))
    cols = pl.BlockSpec((rows, LANES), lambda h: (0, h))
    return pl.pallas_call(
        functools.partial(attend_back_kernel, chunk=chunk),
        grid=(pairs,),
        in_specs=[
            spec(0), spec(1), spec(2), fixed, cols, cols,
            pl.BlockSpec((1, 2, rows), lambda h: (h, 0, 0)), fixed, fixed,
        ],
        out_specs=pl.BlockSpec((3, rows, LANES), lambda h: (0, 0, h)),
        out_shape=jax.ShapeDtypeStruct((3, rows, features), BF),
        scratch_shapes=[pltpu.VMEM((rows, LANES), F32), pltpu.VMEM((rows, LANES), F32)],
        compiler_params=pltpu.CompilerParams(vmem_limit_bytes=VMEM_BYTES),
        name="attend_back",
    )(qkv, qkv, qkv, bias, context, grad_ctx, lse, cos_table, sine_table)


def normalize(hidden, gain_vec, shift_vec):
    row_mean = jnp.mean(hidden, axis=-1, keepdims=True)
    centred = hidden - row_mean
    row_var = jnp.mean(centred * centred, axis=-1, keepdims=True)
    inv_std = lax.rsqrt(row_var + NORM_EPS)
    normed = centred * inv_std
    return (normed * gain_vec + shift_vec, normed, inv_std)


def normalize_back(grad_unit, normed, inv_std):
    first_mean = jnp.mean(grad_unit, axis=-1, keepdims=True)
    second_mean = jnp.mean(grad_unit * normed, axis=-1, keepdims=True)
    return inv_std * (grad_unit - first_mean - normed * second_mean)


def column_sum(values):
    return jnp.sum(values, axis=0, keepdims=True)


def middle_kernel(
    x_ref, ctx_ref, cot_ref, live_ref, attn_ref, ffn_ref, vec_ref, b_up_ref,
    mixed_ref, act_ref, g_up_ref, mid_ref, g_down_ref, g_attn_ref, g_first_ref, g_ctx_ref,
    small_ref, small_up_ref, slope_ref, *, chunk
):
    members, depth, cols = attn_ref.shape[1], attn_ref.shape[2], attn_ref.shape[3]
    ffn_depth, units = ffn_ref.shape[2] // 2, ffn_ref.shape[3]
    b_out, gain_one, shift_one = vec_ref[0:1], vec_ref[1:2], vec_ref[2:3]
    b_down, gain_two, shift_two = vec_ref[3:4], vec_ref[4:5], vec_ref[5:6]

    @pl.when(pl.program_id(0) == 0)
    def _():
        small_ref[...] = jnp.zeros_like(small_ref)
        small_up_ref[...] = jnp.zeros_like(small_up_ref)

    first_sum = x_ref[...].astype(F32) + b_out
    for t in range(members):
        first_sum += dot(ctx_ref[:, t * cols : (t + 1) * cols], block_rows(attn_ref, t, 0, depth), NT)
    normed_one, unit_one, inv_one = normalize(first_sum, gain_one, shift_one)
    mid = normed_one.astype(BF)
    mid_ref[...] = mid
    second_sum = normed_one + b_down
    for t in range(members):
        for start in range(0, units, chunk):
            here = slice(t * units + start, t * units + start + chunk)
            span = slice(start, start + chunk)
            up_proj = dot(mid, block_rows(ffn_ref, t, 0, ffn_depth, span), NN) + b_up_ref[:, here]
            phi = 0.5 * (1.0 + lax.erf(up_proj * INV_ROOT_TWO))
            act_ref[:, here] = (up_proj * phi).astype(BF)
            slope_ref[:, here] = phi + up_proj * jnp.exp(-0.5 * up_proj * up_proj) * INV_ROOT_TAU
        half = slice(t * units, (t + 1) * units)
        second_sum += dot(act_ref[:, half], block_rows(ffn_ref, t, 1, ffn_depth), NT)
    result, unit_two, inv_two = normalize(second_sum, gain_two, shift_two)
    mixed_ref[...] = result.astype(BF)

    grad_out = jnp.where(live_ref[...] > 0.0, cot_ref[...].astype(F32), 0.0)
    grad_second = normalize_back(grad_out * gain_two, unit_two, inv_two)
    small_ref[5:6] += column_sum(grad_out * unit_two)
    small_ref[6:7] += column_sum(grad_out)
    small_ref[4:5] += column_sum(grad_second)
    grad_down = grad_second.astype(BF)
    g_down_ref[...] = grad_down
    grad_mid = grad_second
    for t in range(members):
        for start in range(0, units, chunk):
            here = slice(t * units + start, t * units + start + chunk)
            span = slice(start, start + chunk)
            grad_act = dot(grad_down, block_rows(ffn_ref, t, 1, ffn_depth, span), NN)
            grad_up = (grad_act * slope_ref[:, here]).astype(BF)
            g_up_ref[:, here] = grad_up
            small_up_ref[:, here] += column_sum(grad_up.astype(F32))
        half = slice(t * units, (t + 1) * units)
        grad_mid += dot(g_up_ref[:, half], block_rows(ffn_ref, t, 0, ffn_depth), NT)
    small_ref[2:3] += column_sum(grad_mid * unit_one)
    small_ref[3:4] += column_sum(grad_mid)
    grad_first = normalize_back(grad_mid * gain_one, unit_one, inv_one)
    small_ref[1:2] += column_sum(grad_first)
    g_first_ref[...] = grad_first
    grad_attn = grad_first.astype(BF)
    g_attn_ref[...] = grad_attn
    for t in range(members):
        g_ctx_ref[:, t * cols : (t + 1) * cols] = dot(
            grad_attn, block_rows(attn_ref, t, 0, depth), NN
        ).astype(BF)


def middle(x, context, cotangent, live, attn_w, ffn_w, vectors, b_up):
    rows, features = x.shape
    groups, members, depth4, cols = attn_w.shape
    ffn_rows, units = ffn_w.shape[2], ffn_w.shape[3]
    width = members * units
    tile = 256

    def row(n):
        return pl.BlockSpec((tile, n), lambda i: (i, 0))

    def fixed(shape, index):
        return pl.BlockSpec(shape, lambda i: index, pipeline_mode=pl.Buffered(1))

    def out(n, dtype):
        return jax.ShapeDtypeStruct((rows, n), dtype)

    return pl.pallas_call(
        functools.partial(middle_kernel, chunk=512),
        grid=(rows // tile,),
        in_specs=[
            row(features), row(features), row(features), row(1),
            fixed((groups, members, depth4 // 4, cols), (0, 0, 3, 0)),
            fixed((groups, members, ffn_rows, units), (0, 0, 0, 0)),
            fixed((8, features), (0, 0)), fixed((1, width), (0, 0)),
        ],
        out_specs=[
            row(features), row(width), row(width), row(features), row(features), row(features),
            row(features), row(features),
            pl.BlockSpec((8, features), lambda i: (0, 0)), pl.BlockSpec((1, width), lambda i: (0, 0)),
        ],
        out_shape=[
            out(features, BF), out(width, BF), out(width, BF), out(features, BF), out(features, BF),
            out(features, BF), out(features, F32), out(features, BF),
            jax.ShapeDtypeStruct((8, features), F32), jax.ShapeDtypeStruct((1, width), F32),
        ],
        scratch_shapes=[pltpu.VMEM((tile, width), F32)],
        compiler_params=pltpu.CompilerParams(vmem_limit_bytes=VMEM_BYTES),
        name="middle",
    )(x, context, cotangent, live, attn_w, ffn_w, vectors, b_up)


def ffn_weights_kernel(mid_ref, g_down_ref, act_ref, g_up_ref, out_ref, mid_t_ref, down_t_ref):
    groups, _, depth2, width = out_ref.shape
    depth = depth2 // 2

    @pl.when((pl.program_id(0) == 0) & (pl.program_id(1) == 0))
    def _():
        mid_t_ref[...] = mid_ref[...].T
        down_t_ref[...] = g_down_ref[...].T

    out_ref[:, 0, :depth] = dot(mid_t_ref[...], g_up_ref[...], NN).astype(BF).reshape(groups, depth, width)
    out_ref[:, 0, depth:] = dot(down_t_ref[...], act_ref[...], NN).astype(BF).reshape(groups, depth, width)


def ffn_weights(mid, grad_down, act, grad_up, groups, members):
    rows, features = mid.shape
    units = act.shape[1] // members
    chunk = 512
    per = units // chunk
    fixed = pl.BlockSpec((rows, features), lambda t, j: (0, 0), pipeline_mode=pl.Buffered(1))
    part = pl.BlockSpec((rows, chunk), lambda t, j: (0, t * per + j))
    depth2 = 2 * features // groups
    return pl.pallas_call(
        ffn_weights_kernel,
        grid=(members, per),
        in_specs=[fixed, fixed, part, part],
        out_specs=pl.BlockSpec((groups, 1, depth2, chunk), lambda t, j: (0, t, 0, j)),
        out_shape=jax.ShapeDtypeStruct((groups, members, depth2, units), BF),
        scratch_shapes=[pltpu.VMEM((features, rows), BF), pltpu.VMEM((features, rows), BF)],
        compiler_params=pltpu.CompilerParams(vmem_limit_bytes=VMEM_BYTES),
        name="ffn_weights",
    )(mid, grad_down, act, grad_up)


def attn_weights_kernel(
    x_ref, g_attn_ref, ctx_ref, raw_ref, w_ref, g_first_ref, out_ref, rows_ref, bias_ref,
    x_t_ref, attn_t_ref, sum_ref
):
    groups, _, depth4, cols = out_ref.shape
    depth = depth4 // 4
    step = pl.program_id(0)

    @pl.when(step == 0)
    def _():
        x_t_ref[...] = x_ref[...].T
        attn_t_ref[...] = g_attn_ref[...].T
        sum_ref[...] = g_first_ref[...]
        bias_ref[...] = jnp.zeros_like(bias_ref)

    total = sum_ref[...]
    for p in range(3):
        out_ref[:, 0, p * depth : (p + 1) * depth] = dot(x_t_ref[...], raw_ref[p], NN).astype(BF).reshape(
            groups, depth, cols
        )
        total += dot(raw_ref[p], block_rows(w_ref, 0, p, depth), NT)
        bias_ref[p : p + 1] = column_sum(raw_ref[p].astype(F32))
    out_ref[:, 0, 3 * depth :] = dot(attn_t_ref[...], ctx_ref[...], NN).astype(BF).reshape(
        groups, depth, cols
    )
    sum_ref[...] = total

    @pl.when(step == pl.num_programs(0) - 1)
    def _():
        rows_ref[...] = sum_ref[...].astype(BF)


def attn_weights(x, grad_attn, context, grad_raw, attn_w, grad_first):
    rows, features = x.shape
    groups, members, depth4, cols = attn_w.shape

    def fixed(n):
        return pl.BlockSpec((rows, n), lambda t: (0, 0), pipeline_mode=pl.Buffered(1))

    return pl.pallas_call(
        attn_weights_kernel,
        grid=(members,),
        in_specs=[
            fixed(features), fixed(features), pl.BlockSpec((rows, cols), lambda t: (0, t)),
            pl.BlockSpec((3, rows, cols), lambda t: (0, 0, t)),
            pl.BlockSpec((groups, 1, depth4, cols), lambda t: (0, t, 0, 0)), fixed(features),
        ],
        out_specs=[
            pl.BlockSpec((groups, 1, depth4, cols), lambda t: (0, t, 0, 0)),
            pl.BlockSpec((rows, features), lambda t: (0, 0)),
            pl.BlockSpec((8, cols), lambda t: (0, t)),
        ],
        out_shape=[
            jax.ShapeDtypeStruct((groups, members, depth4, cols), BF),
            jax.ShapeDtypeStruct((rows, features), BF),
            jax.ShapeDtypeStruct((8, features), F32),
        ],
        scratch_shapes=[
            pltpu.VMEM((features, rows), BF), pltpu.VMEM((features, rows), BF),
            pltpu.VMEM((rows, features), F32),
        ],
        compiler_params=pltpu.CompilerParams(vmem_limit_bytes=VMEM_BYTES),
        name="attn_weights",
    )(x, grad_attn, context, grad_raw, attn_w, grad_first)


def merge_groups(w, parts):
    groups, members, rows, cols = w.shape
    depth = rows // parts
    if depth % 16 == 0:
        return w
    w = w.reshape(groups, members, parts, depth, cols).transpose(1, 2, 0, 3, 4)
    return w.reshape(1, members, parts * groups * depth, cols)


def split_groups(w, parts, groups):
    have, members, rows, cols = w.shape
    if have == groups:
        return w
    w = w.reshape(members, parts, groups, rows // parts // groups, cols).transpose(2, 0, 1, 3, 4)
    return w.reshape(groups, members, rows // groups, cols)


def layer(rows, cotangent, place, length, cos_table, sine_table, attn_w, ffn_w, b_qkv, b_up, vectors):
    live = place < length
    bias = jnp.broadcast_to(jnp.where(live, 0.0, MASK_FILL).astype(BF)[:, None], (rows.shape[0], LANES))
    qkv = project(rows, attn_w, b_qkv[:, None, :], cos_table, sine_table)
    context, lse = attend(qkv, bias)
    mixed, act, g_up, mid, g_down, g_attn, g_first, g_ctx, small, small_up = middle(
        rows, context, cotangent, live.astype(F32)[:, None], attn_w, ffn_w, vectors, b_up
    )
    g_ffn = ffn_weights(mid, g_down, act, g_up, ffn_w.shape[0], ffn_w.shape[1])
    g_raw = attend_back(qkv, bias, context, g_ctx, lse, cos_table, sine_table)
    g_attn_w, grad_rows, small_qkv = attn_weights(rows, g_attn, context, g_raw, attn_w, g_first)
    packed = jnp.concatenate([small_qkv[:3], small[1:7], small_up.reshape(-1, small.shape[1])], axis=0)
    return mixed, grad_rows, g_attn_w, g_ffn, packed


MESH = pl.DeviceIdType.MESH


def axis_orders(bits, rows):
    core = bits - 2
    rest = [d for d in range(bits) if d != core]
    if bits != 5 or rows % 192:
        return [(0, rows, tuple(rest) + (core,))]
    far, near, y, _, x = range(5)
    unit = rows // 12
    return [
        (0, 5 * unit, (far, near, x, y, core)),
        (5 * unit, 5 * unit, (far, near, y, x, core)),
        (10 * unit, 2 * unit, (x, y, near, far, core)),
    ]


class Place:
    def __init__(self, devices, members):
        self.devices, self.members = devices, members
        self.bits = devices.bit_length() - 1
        self.me = lax.axis_index("dp") * members + lax.axis_index("tensor")
        self.bit = [self.me // self.stride(d) % 2 for d in range(self.bits)]

    def stride(self, dim):
        return 1 << (self.bits - 1 - dim)

    def ident(self, number):
        return (number // self.members, number % self.members)

    def partner(self, dim):
        return self.ident(self.me + (1 - 2 * self.bit[dim]) * self.stride(dim))

    def meet_all(self):
        barrier = pltpu.get_barrier_semaphore()

        def greet(offset, carry):
            pl.semaphore_signal(
                barrier, inc=1, device_id=self.ident((self.me + offset) % self.devices),
                device_id_type=MESH,
            )
            return carry

        lax.fori_loop(1, self.devices, greet, 0)
        pl.semaphore_wait(barrier, self.devices - 1)

    def swap(self, src, dst, send_sem, recv_sem, offset):
        target = (self.me + offset) % self.devices
        return pltpu.make_async_remote_copy(
            src_ref=src.at[target], dst_ref=dst.at[self.me], send_sem=send_sem.at[offset],
            recv_sem=recv_sem.at[offset], device_id=self.ident(target), device_id_type=MESH,
        )

    def for_others(self, action):
        def one(offset, carry):
            action(offset)
            return carry

        lax.fori_loop(1, self.devices, one, 0)


def head_kernel(
    rows_ref, shard_ref, bias_ref, seq_ref, attn_ref, biases_ref, held_ref,
    send_sem, recv_sem, w_send, w_recv, b_sem, local_sem, *, devices, members
):
    here = Place(devices, members)
    bits = here.bits
    colours = axis_orders(bits, shard_ref.shape[0])
    mine = pltpu.make_async_copy(rows_ref.at[here.me], held_ref, local_sem.at[0])
    mine.start()
    own = pltpu.make_async_copy(shard_ref, attn_ref.at[tuple(here.bit)], local_sem.at[1])
    own.start()
    own_bias = pltpu.make_async_copy(bias_ref, biases_ref.at[here.me % members], local_sem.at[2])
    own_bias.start()
    here.meet_all()

    def spread(colour, step):
        start, count, order = colours[colour]
        done = set(order[:step])
        span = pl.ds(start, count)
        place = tuple(slice(None) if d in done else here.bit[d] for d in range(bits))
        there = attn_ref.at[place + (span, slice(None))]
        return pltpu.make_async_remote_copy(
            src_ref=shard_ref.at[span] if step == 0 else there, dst_ref=there,
            send_sem=w_send.at[colour, step], recv_sem=w_recv.at[colour, step],
            device_id=here.partner(order[step]), device_id_type=MESH,
        )

    to_member = pltpu.make_async_remote_copy(
        src_ref=bias_ref, dst_ref=biases_ref.at[here.me % members], send_sem=b_sem.at[0],
        recv_sem=b_sem.at[1], device_id=here.partner(bits - 1), device_id_type=MESH,
    )
    moving = [spread(c, 0) for c in range(len(colours))]
    for copy in moving:
        copy.start()
    to_member.start()
    here.for_others(lambda o: here.swap(rows_ref, seq_ref, send_sem, recv_sem, o).start())
    mine.wait()
    back = pltpu.make_async_copy(held_ref, seq_ref.at[here.me], local_sem.at[0])
    back.start()
    own.wait()
    own_bias.wait()
    for step in range(bits):
        for c in range(len(colours)):
            moving[c].wait()
            if step + 1 < bits:
                moving[c] = spread(c, step + 1)
                moving[c].start()
    to_member.wait()
    back.wait()
    here.for_others(lambda o: here.swap(rows_ref, seq_ref, send_sem, recv_sem, o).wait())


def head(tokens, attn_shard, biases, members):
    devices, stripe, features = tokens.shape
    bits = devices.bit_length() - 1
    colours = len(axis_orders(bits, attn_shard.shape[0]))
    anywhere = pl.BlockSpec(memory_space=pl.ANY)
    onchip = pl.BlockSpec(memory_space=pltpu.VMEM)
    sems = pltpu.SemaphoreType.DMA
    seq, attn, both = pl.pallas_call(
        functools.partial(head_kernel, devices=devices, members=members),
        in_specs=[anywhere, onchip, onchip],
        out_specs=[anywhere, anywhere, anywhere],
        out_shape=[
            jax.ShapeDtypeStruct(tokens.shape, BF),
            jax.ShapeDtypeStruct((2,) * bits + attn_shard.shape, BF),
            jax.ShapeDtypeStruct((members,) + biases.shape, F32),
        ],
        scratch_shapes=[
            pltpu.VMEM((stripe, features), BF), sems((devices,)), sems((devices,)),
            sems((colours, bits)), sems((colours, bits)), sems((2,)), sems((3,)),
        ],
        compiler_params=pltpu.CompilerParams(collective_id=0, has_side_effects=True),
        name="head",
    )(tokens, attn_shard, biases)
    return seq, attn.reshape((devices,) + attn_shard.shape), both


def tail_kernel(
    rows_ref, grad_ref, small_ref, back_ref, sum_ref, total_ref, held_ref, *rest, devices, members
):
    here = Place(devices, members)
    bits = here.bits
    colours = axis_orders(bits, grad_ref.shape[-2])
    count = len(colours)
    got = [rest[c * bits : (c + 1) * bits] for c in range(count)]
    kept = [rest[(count + c) * bits : (count + c + 1) * bits] for c in range(count)]
    small_got, small_kept = rest[2 * count * bits : 2 * count * bits + 2]
    send_sem, recv_sem, w_send, w_recv, s_send, s_recv, local_sem = rest[2 * count * bits + 2 :]
    mine = pltpu.make_async_copy(rows_ref.at[here.me], held_ref, local_sem.at[0])
    mine.start()
    here.meet_all()

    def current(colour, step):
        start, size, _ = colours[colour]
        if step == 0:
            return grad_ref, (pl.ds(start, size), slice(None))
        return kept[colour][step - 1], (slice(None), slice(None))

    def place(colour, step, side):
        order = colours[colour][2][::-1]
        left = [d for d in range(bits) if d not in order[:step]]
        return tuple(
            (here.bit[d] if side else 1 - here.bit[d]) if d == order[step] else slice(None)
            for d in left
        )

    def hand_over(colour, step):
        ref, inner = current(colour, step)
        return pltpu.make_async_remote_copy(
            src_ref=ref.at[place(colour, step, False) + inner], dst_ref=got[colour][step],
            send_sem=w_send.at[colour, step], recv_sem=w_recv.at[colour, step],
            device_id=here.partner(colours[colour][2][::-1][step]), device_id_type=MESH,
        )

    def hand_small(step):
        return pltpu.make_async_remote_copy(
            src_ref=small_ref if step == 0 else small_kept.at[step - 1], dst_ref=small_got.at[step],
            send_sem=s_send.at[step], recv_sem=s_recv.at[step],
            device_id=here.partner(bits - 1 - step), device_id_type=MESH,
        )

    moving = [hand_over(c, 0) for c in range(count)]
    for copy in moving:
        copy.start()
    small = hand_small(0)
    small.start()
    here.for_others(lambda o: here.swap(rows_ref, back_ref, send_sem, recv_sem, o).start())
    mine.wait()
    back = pltpu.make_async_copy(held_ref, back_ref.at[here.me], local_sem.at[0])
    back.start()
    for step in range(bits):
        for c in range(count):
            moving[c].wait()
            ref, inner = current(c, step)
            added = ref[place(c, step, True) + inner] + got[c][step][...]
            if step + 1 < bits:
                kept[c][step][...] = added
                moving[c] = hand_over(c, step + 1)
                moving[c].start()
            else:
                start, size, _ = colours[c]
                sum_ref[start : start + size] = added.astype(F32)
        small.wait()
        before = small_ref[...] if step == 0 else small_kept[step - 1]
        after = before + small_got[step]
        if step + 1 < bits:
            small_kept[step] = after
            small = hand_small(step + 1)
            small.start()
        else:
            total_ref[...] = after
    back.wait()
    here.for_others(lambda o: here.swap(rows_ref, back_ref, send_sem, recv_sem, o).wait())


def tail(grad_rows, grad_w, small, members):
    devices, stripe, features = grad_rows.shape
    bits = devices.bit_length() - 1
    rows, cols = grad_w.shape[1:]
    colours = axis_orders(bits, rows)
    anywhere = pl.BlockSpec(memory_space=pl.ANY)
    onchip = pl.BlockSpec(memory_space=pltpu.VMEM)
    sems = pltpu.SemaphoreType.DMA
    levels = [
        pltpu.VMEM((2,) * (bits - 1 - step) + (size, cols), BF)
        for _, size, _ in colours
        for step in range(bits)
    ]
    return pl.pallas_call(
        functools.partial(tail_kernel, devices=devices, members=members),
        in_specs=[anywhere, onchip, onchip],
        out_specs=[anywhere, onchip, onchip],
        out_shape=[
            jax.ShapeDtypeStruct(grad_rows.shape, BF),
            jax.ShapeDtypeStruct((rows, cols), F32),
            jax.ShapeDtypeStruct(small.shape, F32),
        ],
        scratch_shapes=[pltpu.VMEM((stripe, features), BF)] + levels + levels + [
            pltpu.VMEM((bits,) + small.shape, F32), pltpu.VMEM((bits,) + small.shape, F32),
            sems((devices,)), sems((devices,)), sems((len(colours), bits)), sems((len(colours), bits)),
            sems((bits,)), sems((bits,)), sems((1,)),
        ],
        compiler_params=pltpu.CompilerParams(
            collective_id=1, has_side_effects=True, vmem_limit_bytes=VMEM_BYTES
        ),
        name="tail",
    )(grad_rows, grad_w.reshape((2,) * bits + (rows, cols)), small)


def body(
    tokens, out_grad, lengths, order, w_qkv, b_qkv, w_out, b_out, norm1_gain, norm1_bias,
    w_up, b_up, w_down, b_down, norm2_gain, norm2_bias,
):
    dp_size = lax.axis_size("dp")
    tp_size = lax.axis_size("tensor")
    devices = dp_size * tp_size
    me = lax.axis_index(AXES)
    stored, stripe, features = tokens.shape
    slot = devices * stripe
    depth = w_qkv.shape[1]
    cols = w_qkv.shape[2]
    units = w_up.shape[1]

    def deal(rows_val):
        return lax.all_to_all(rows_val, AXES, split_axis=0, concat_axis=0, tiled=True)

    ffn_shard = jnp.concatenate([w_up, w_down.T], axis=0)
    ffn_all = lax.all_gather(ffn_shard, AXES, axis=0, tiled=True)
    ffn_w = merge_groups(ffn_all.reshape(dp_size, tp_size, 2 * depth, units), 2)
    attn_shard = jnp.concatenate([w_qkv.reshape(3 * depth, cols), w_out.T], axis=0)
    biases = jnp.concatenate([b_qkv.reshape(-1), b_up]).reshape(-1, LANES)
    rows, attn_all, biases = head(tokens, attn_shard, biases, tp_size)
    rows = rows.reshape(slot, features)
    attn_w = merge_groups(attn_all.reshape(dp_size, tp_size, 4 * depth, cols), 4)
    biases = biases.reshape(tp_size, -1)
    b_qkv_all = biases[:, : 3 * cols].reshape(tp_size, 3, cols).transpose(1, 0, 2).reshape(3, features)
    b_up_all = biases[:, 3 * cols :].reshape(1, tp_size * units)
    cotangent = deal(out_grad).reshape(slot, features)
    cos_table, sine_table = rope_tables(order)
    none = jnp.zeros_like(b_out)
    vectors = jnp.stack(
        [b_out, norm1_gain, norm1_bias, b_down, norm2_gain, norm2_bias, none, none], axis=0
    )
    length = lax.dynamic_index_in_dim(lengths, me, 0, keepdims=False)
    result, grad_rows, g_attn_w, g_ffn, packed = layer(
        rows, cotangent, order, length, cos_table, sine_table, attn_w, ffn_w, b_qkv_all, b_up_all, vectors
    )
    mixed = deal(result.reshape(devices, stripe, features))
    laid = split_groups(g_ffn, 2, dp_size).reshape(devices * 2 * depth, units)
    ffn_sum = lax.psum_scatter(laid, AXES, scatter_dimension=0, tiled=True).astype(F32)
    laid = split_groups(g_attn_w, 4, dp_size).reshape(devices, 4 * depth, cols)
    packed = jnp.pad(packed, ((0, -packed.shape[0] % 8), (0, 0)))
    grad_tokens, attn_sum, summed = tail(
        grad_rows.reshape(devices, stripe, features), laid, packed, tp_size
    )
    return (
        mixed, grad_tokens, attn_sum[: 3 * depth].reshape(3, depth, cols), summed[:3],
        attn_sum[3 * depth :].T, summed[3], summed[4], summed[5], ffn_sum[:depth],
        summed[9:13].reshape(-1), ffn_sum[depth:].T, summed[6], summed[7], summed[8],
    )


def solution(mesh):
    rows = P(None, AXES, None)
    in_specs = (
        rows, rows, P(), P(), P(None, "dp", "tensor"), P(None, "tensor"), P("tensor", "dp"), P(),
        P(), P(), P("dp", "tensor"), P("tensor"), P("tensor", "dp"), P(), P(), P(),
    )
    out_specs = (
        rows, rows, P(None, "dp", "tensor"), P(), P("tensor", "dp"), P(), P(), P(),
        P("dp", "tensor"), P(), P("tensor", "dp"), P(), P(), P(),
    )
    return jax.shard_map(body, mesh=mesh, in_specs=in_specs, out_specs=out_specs, check_vma=False)
```

```python
import functools

import jax
import jax.numpy as jnp
from jax import lax
from jax.experimental import pallas as pl
from jax.experimental.pallas import tpu as pltpu
from jax.sharding import PartitionSpec as P

HD = 64
LANES = 128
NORM_EPS = 1e-12
ROPE_BASE = 10000.0
MASK_FILL = -1e30
SCORE_SCALE = 0.125
INV_ROOT_TWO = 0.7071067811865476
INV_ROOT_TAU = 0.3989422804014327
AXES = ("dp", "tensor")
BF = jnp.bfloat16
F32 = jnp.float32
VMEM_BYTES = 60 * 1024 * 1024


def dot(a, b, dims):
    return lax.dot_general(a, b, (dims, ((), ())), preferred_element_type=F32)


NN = ((1,), (0,))
NT = ((1,), (1,))
TN = ((0,), (0,))


def inverse_steps():
    steps = (jnp.arange(LANES) % HD // 2).astype(F32)
    return jnp.power(ROPE_BASE, -2.0 * steps / HD)[None, :]


def turn(values, cos_table, sine_table):
    lane = lax.broadcasted_iota(jnp.int32, values.shape, 1)
    swapped = jnp.where(
        lane % 2 == 0, -pltpu.roll(values, LANES - 1, 1), pltpu.roll(values, 1, 1)
    )
    return values * cos_table + swapped * sine_table


def block_rows(w_ref, member, part, depth, cols=slice(None)):
    taken = w_ref[:, member, part * depth : (part + 1) * depth, cols]
    return taken.reshape(taken.shape[0] * depth, taken.shape[2])


def project_kernel(x_ref, w_ref, b_ref, cos_ref, sine_ref, out_ref):
    kind = pl.program_id(0)
    depth = w_ref.shape[2]
    weight = [block_rows(w_ref, t, 0, depth) for t in range(w_ref.shape[1])]
    raw = dot(x_ref[...], jnp.concatenate(weight, axis=1), NN) + b_ref[0]

    @pl.when(kind < 2)
    def _():
        for part in range(raw.shape[1] // LANES):
            cols = slice(part * LANES, (part + 1) * LANES)
            out_ref[0, :, cols] = turn(raw[:, cols], cos_ref[...], sine_ref[...]).astype(BF)

    @pl.when(kind == 2)
    def _():
        out_ref[0] = raw.astype(BF)


def project(x, attn_w, b, cos_table, sine_table):
    rows, features = x.shape
    groups, members, depth4, cols = attn_w.shape
    depth = depth4 // 4
    tile = rows // 2
    return pl.pallas_call(
        project_kernel,
        grid=(3, rows // tile),
        in_specs=[
            pl.BlockSpec((tile, features), lambda p, r: (r, 0)),
            pl.BlockSpec((groups, members, depth, cols), lambda p, r: (0, 0, p, 0)),
            pl.BlockSpec((1, 1, features), lambda p, r: (p, 0, 0)),
            pl.BlockSpec((tile, LANES), lambda p, r: (r, 0)),
            pl.BlockSpec((tile, LANES), lambda p, r: (r, 0)),
        ],
        out_specs=pl.BlockSpec((1, tile, features), lambda p, r: (p, r, 0)),
        out_shape=jax.ShapeDtypeStruct((3, rows, features), BF),
        compiler_params=pltpu.CompilerParams(vmem_limit_bytes=VMEM_BYTES),
        name="project",
    )(x, attn_w, b, cos_table, sine_table)


def pair_operands(q, k, bias, lane, head):
    inside = lane // HD == head
    spare = lane == (1 - head) * HD
    zero = jnp.zeros_like(q)
    q_head = jnp.where(inside, q, jnp.where(spare, jnp.ones_like(q), zero))
    k_head = jnp.where(inside, k, jnp.where(spare, bias, zero))
    return q_head, k_head


def attend_kernel(q_ref, k_ref, v_ref, bias_ref, ctx_ref, lse_ref, *, chunk):
    rows = q_ref.shape[1]
    lane = lax.broadcasted_iota(jnp.int32, (rows, LANES), 1)
    q = q_ref[0] * jnp.asarray(SCORE_SCALE, BF)
    k = k_ref[0]
    v_turned = v_ref[0].T
    ones = jnp.ones((16, rows), BF)
    v_heads = [
        jnp.concatenate([v_turned[head * HD : (head + 1) * HD], ones], axis=0) for head in range(2)
    ]
    bias = bias_ref[...]
    for part in range(rows // chunk):
        span = slice(part * chunk, (part + 1) * chunk)
        outs = []
        for head in range(2):
            q_head, k_head = pair_operands(q, k, bias, lane, head)
            scores = dot(k_head, q_head[span], NT)
            tops = jnp.max(scores.reshape(16, rows // 16, chunk), axis=0)
            top = jnp.max(tops, axis=0, keepdims=True)
            expo = jnp.exp(scores - top)
            mixed = dot(v_heads[head], expo.astype(BF), NN)
            total = mixed[HD : HD + 1]
            outs.append(mixed[:HD] / total)
            lse_ref[0, head : head + 1, span] = top + jnp.log(total)
        ctx_ref[span, :] = jnp.concatenate(outs, axis=0).T.astype(BF)


def attend(qkv, bias):
    _, rows, features = qkv.shape
    pairs = features // LANES
    chunk = rows

    def spec(which):
        return pl.BlockSpec((1, rows, LANES), lambda h: (which, 0, h))

    return pl.pallas_call(
        functools.partial(attend_kernel, chunk=chunk),
        grid=(pairs,),
        in_specs=[spec(0), spec(1), spec(2), pl.BlockSpec((rows, LANES), lambda h: (0, 0))],
        out_specs=[
            pl.BlockSpec((rows, LANES), lambda h: (0, h)),
            pl.BlockSpec((1, 2, rows), lambda h: (h, 0, 0)),
        ],
        out_shape=[
            jax.ShapeDtypeStruct((rows, features), BF),
            jax.ShapeDtypeStruct((pairs, 2, rows), F32),
        ],
        compiler_params=pltpu.CompilerParams(vmem_limit_bytes=VMEM_BYTES),
        name="attend",
    )(qkv, qkv, qkv, bias)


def attend_back_kernel(
    q_ref, k_ref, v_ref, bias_ref, ctx_ref, grad_ref, lse_ref, cos_ref, sine_ref, out_ref,
    dk_ref, dv_ref, *, chunk
):
    rows = q_ref.shape[1]
    lane = lax.broadcasted_iota(jnp.int32, (rows, LANES), 1)
    q = q_ref[0] * jnp.asarray(SCORE_SCALE, BF)
    k = k_ref[0]
    v = v_ref[0]
    grad = grad_ref[...]
    bias = bias_ref[...]
    k_turned = k.T
    zero = jnp.zeros_like(grad)
    dots = (grad.astype(F32) * ctx_ref[...].astype(F32)).T
    for part in range(rows // chunk):
        span = slice(part * chunk, (part + 1) * chunk)
        dq_parts = []
        dk_sum = None
        dv_sum = None
        for head in range(2):
            q_head, k_head = pair_operands(q, k, bias, lane, head)
            inside = lane // HD == head
            g_head = jnp.where(inside, grad, zero)[span]
            q_only = jnp.where(inside, q, zero)[span]
            scores = dot(k_head, q_head[span], NT)
            prob = jnp.exp(scores - lse_ref[0, head : head + 1, span])
            g_prob = dot(v, g_head, NT)
            inner = jnp.sum(dots[head * HD : (head + 1) * HD, span], axis=0, keepdims=True)
            g_score = (prob * (g_prob - inner)).astype(BF)
            dv = dot(prob.astype(BF), g_head, NN)
            dk = dot(g_score, q_only, NN)
            dq_parts.append(dot(k_turned[head * HD : (head + 1) * HD], g_score, NN))
            dk_sum = dk if dk_sum is None else dk_sum + dk
            dv_sum = dv if dv_sum is None else dv_sum + dv
        dq = jnp.concatenate(dq_parts, axis=0).T * SCORE_SCALE
        out_ref[0, span, :] = turn(dq, cos_ref[span, :], -sine_ref[span, :]).astype(BF)
        if part == 0:
            dk_ref[...] = dk_sum
            dv_ref[...] = dv_sum
        else:
            dk_ref[...] += dk_sum
            dv_ref[...] += dv_sum
    out_ref[1] = turn(dk_ref[...], cos_ref[...], -sine_ref[...]).astype(BF)
    out_ref[2] = dv_ref[...].astype(BF)


def attend_back(qkv, bias, context, grad_ctx, lse, cos_table, sine_table):
    _, rows, features = qkv.shape
    pairs = features // LANES
    chunk = 256

    def spec(which):
        return pl.BlockSpec((1, rows, LANES), lambda h: (which, 0, h))

    fixed = pl.BlockSpec((rows, LANES), lambda h: (0, 0))
    cols = pl.BlockSpec((rows, LANES), lambda h: (0, h))
    return pl.pallas_call(
        functools.partial(attend_back_kernel, chunk=chunk),
        grid=(pairs,),
        in_specs=[
            spec(0), spec(1), spec(2), fixed, cols, cols,
            pl.BlockSpec((1, 2, rows), lambda h: (h, 0, 0)), fixed, fixed,
        ],
        out_specs=pl.BlockSpec((3, rows, LANES), lambda h: (0, 0, h)),
        out_shape=jax.ShapeDtypeStruct((3, rows, features), BF),
        scratch_shapes=[pltpu.VMEM((rows, LANES), F32), pltpu.VMEM((rows, LANES), F32)],
        compiler_params=pltpu.CompilerParams(vmem_limit_bytes=VMEM_BYTES),
        name="attend_back",
    )(qkv, qkv, qkv, bias, context, grad_ctx, lse, cos_table, sine_table)


def normalize(hidden, gain_vec, shift_vec):
    row_mean = jnp.mean(hidden, axis=-1, keepdims=True)
    centred = hidden - row_mean
    row_var = jnp.mean(centred * centred, axis=-1, keepdims=True)
    inv_std = lax.rsqrt(row_var + NORM_EPS)
    normed = centred * inv_std
    return (normed * gain_vec + shift_vec, normed, inv_std)


def normalize_back(grad_unit, normed, inv_std):
    first_mean = jnp.mean(grad_unit, axis=-1, keepdims=True)
    second_mean = jnp.mean(grad_unit * normed, axis=-1, keepdims=True)
    return inv_std * (grad_unit - first_mean - normed * second_mean)


def column_sum(values):
    rows = values.shape[0]
    grouped = jnp.sum(values.reshape(rows // 32, 32, values.shape[1]), axis=0)
    return jnp.sum(grouped, axis=0, keepdims=True)


def middle_kernel(
    x_ref, ctx_ref, cot_ref, live_ref, attn_ref, ffn_ref, vec_ref, b_up_ref,
    mixed_ref, act_ref, g_up_ref, mid_ref, g_down_ref, g_attn_ref, g_first_ref, g_ctx_ref,
    small_ref, small_up_ref, slope_ref, *, chunk
):
    members, depth, cols = attn_ref.shape[1], attn_ref.shape[2], attn_ref.shape[3]
    ffn_depth, units = ffn_ref.shape[2] // 2, ffn_ref.shape[3]
    b_out, gain_one, shift_one = vec_ref[0:1], vec_ref[1:2], vec_ref[2:3]
    b_down, gain_two, shift_two = vec_ref[3:4], vec_ref[4:5], vec_ref[5:6]

    @pl.when(pl.program_id(0) == 0)
    def _():
        small_ref[...] = jnp.zeros_like(small_ref)
        small_up_ref[...] = jnp.zeros_like(small_up_ref)

    first_sum = x_ref[...].astype(F32) + b_out
    for t in range(members):
        first_sum += dot(ctx_ref[:, t * cols : (t + 1) * cols], block_rows(attn_ref, t, 0, depth), NT)
    normed_one, unit_one, inv_one = normalize(first_sum, gain_one, shift_one)
    mid = normed_one.astype(BF)
    mid_ref[...] = mid
    second_sum = normed_one + b_down
    for t in range(members):
        for start in range(0, units, chunk):
            here = slice(t * units + start, t * units + start + chunk)
            span = slice(start, start + chunk)
            up_proj = dot(mid, block_rows(ffn_ref, t, 0, ffn_depth, span), NN) + b_up_ref[:, here]
            phi = 0.5 * (1.0 + lax.erf(up_proj * INV_ROOT_TWO))
            act_ref[:, here] = (up_proj * phi).astype(BF)
            slope_ref[:, here] = phi + up_proj * jnp.exp(-0.5 * up_proj * up_proj) * INV_ROOT_TAU
        half = slice(t * units, (t + 1) * units)
        second_sum += dot(act_ref[:, half], block_rows(ffn_ref, t, 1, ffn_depth), NT)
    result, unit_two, inv_two = normalize(second_sum, gain_two, shift_two)
    mixed_ref[...] = result.astype(BF)

    grad_out = jnp.where(live_ref[:, 0:1].astype(F32) == 0.0, cot_ref[...].astype(F32), 0.0)
    grad_second = normalize_back(grad_out * gain_two, unit_two, inv_two)
    small_ref[5:6] += column_sum(grad_out * unit_two)
    small_ref[6:7] += column_sum(grad_out)
    small_ref[4:5] += column_sum(grad_second)
    grad_down = grad_second.astype(BF)
    g_down_ref[...] = grad_down
    grad_mid = grad_second
    for t in range(members):
        for start in range(0, units, chunk):
            here = slice(t * units + start, t * units + start + chunk)
            span = slice(start, start + chunk)
            grad_act = dot(grad_down, block_rows(ffn_ref, t, 1, ffn_depth, span), NN)
            grad_up = (grad_act * slope_ref[:, here]).astype(BF)
            g_up_ref[:, here] = grad_up
            small_up_ref[:, here] += column_sum(grad_up.astype(F32))
        half = slice(t * units, (t + 1) * units)
        grad_mid += dot(g_up_ref[:, half], block_rows(ffn_ref, t, 0, ffn_depth), NT)
    small_ref[2:3] += column_sum(grad_mid * unit_one)
    small_ref[3:4] += column_sum(grad_mid)
    grad_first = normalize_back(grad_mid * gain_one, unit_one, inv_one)
    small_ref[1:2] += column_sum(grad_first)
    g_first_ref[...] = grad_first
    grad_attn = grad_first.astype(BF)
    g_attn_ref[...] = grad_attn
    for t in range(members):
        g_ctx_ref[:, t * cols : (t + 1) * cols] = dot(
            grad_attn, block_rows(attn_ref, t, 0, depth), NN
        ).astype(BF)


def middle(x, context, cotangent, live, attn_w, ffn_w, vectors, b_up):
    rows, features = x.shape
    groups, members, depth4, cols = attn_w.shape
    ffn_rows, units = ffn_w.shape[2], ffn_w.shape[3]
    width = members * units
    tile = 256

    def row(n):
        return pl.BlockSpec((tile, n), lambda i: (i, 0))

    def fixed(shape, index):
        return pl.BlockSpec(shape, lambda i: index, pipeline_mode=pl.Buffered(1))

    def out(n, dtype):
        return jax.ShapeDtypeStruct((rows, n), dtype)

    return pl.pallas_call(
        functools.partial(middle_kernel, chunk=512),
        grid=(rows // tile,),
        in_specs=[
            row(features), row(features), row(features), row(LANES),
            fixed((groups, members, depth4 // 4, cols), (0, 0, 3, 0)),
            fixed((groups, members, ffn_rows, units), (0, 0, 0, 0)),
            fixed((8, features), (0, 0)), fixed((1, width), (0, 0)),
        ],
        out_specs=[
            row(features), row(width), row(width), row(features), row(features), row(features),
            row(features), row(features),
            pl.BlockSpec((8, features), lambda i: (0, 0)), pl.BlockSpec((1, width), lambda i: (0, 0)),
        ],
        out_shape=[
            out(features, BF), out(width, BF), out(width, BF), out(features, BF), out(features, BF),
            out(features, BF), out(features, F32), out(features, BF),
            jax.ShapeDtypeStruct((8, features), F32), jax.ShapeDtypeStruct((1, width), F32),
        ],
        scratch_shapes=[pltpu.VMEM((tile, width), F32)],
        compiler_params=pltpu.CompilerParams(vmem_limit_bytes=VMEM_BYTES),
        name="middle",
    )(x, context, cotangent, live, attn_w, ffn_w, vectors, b_up)


def ffn_weights_kernel(mid_ref, g_down_ref, act_ref, g_up_ref, out_ref, mid_t_ref, down_t_ref):
    groups, _, depth2, width = out_ref.shape
    depth = depth2 // 2

    @pl.when((pl.program_id(0) == 0) & (pl.program_id(1) == 0))
    def _():
        mid_t_ref[...] = mid_ref[...].T
        down_t_ref[...] = g_down_ref[...].T

    out_ref[:, 0, :depth] = dot(mid_t_ref[...], g_up_ref[...], NN).astype(BF).reshape(groups, depth, width)
    out_ref[:, 0, depth:] = dot(down_t_ref[...], act_ref[...], NN).astype(BF).reshape(groups, depth, width)


def ffn_weights(mid, grad_down, act, grad_up, groups, members):
    rows, features = mid.shape
    units = act.shape[1] // members
    chunk = 512
    per = units // chunk
    fixed = pl.BlockSpec((rows, features), lambda t, j: (0, 0), pipeline_mode=pl.Buffered(1))
    part = pl.BlockSpec((rows, chunk), lambda t, j: (0, t * per + j))
    depth2 = 2 * features // groups
    return pl.pallas_call(
        ffn_weights_kernel,
        grid=(members, per),
        in_specs=[fixed, fixed, part, part],
        out_specs=pl.BlockSpec((groups, 1, depth2, chunk), lambda t, j: (0, t, 0, j)),
        out_shape=jax.ShapeDtypeStruct((groups, members, depth2, units), BF),
        scratch_shapes=[pltpu.VMEM((features, rows), BF), pltpu.VMEM((features, rows), BF)],
        compiler_params=pltpu.CompilerParams(vmem_limit_bytes=VMEM_BYTES),
        name="ffn_weights",
    )(mid, grad_down, act, grad_up)


def attn_weights_kernel(
    x_ref, g_attn_ref, ctx_ref, raw_ref, w_ref, g_first_ref, out_ref, rows_ref, bias_ref,
    x_t_ref, attn_t_ref, sum_ref
):
    groups, _, depth4, cols = out_ref.shape
    depth = depth4 // 4
    step = pl.program_id(0)

    @pl.when(step == 0)
    def _():
        x_t_ref[...] = x_ref[...].T
        attn_t_ref[...] = g_attn_ref[...].T
        sum_ref[...] = g_first_ref[...]
        bias_ref[...] = jnp.zeros_like(bias_ref)

    total = sum_ref[...]
    for p in range(3):
        out_ref[:, 0, p * depth : (p + 1) * depth] = dot(x_t_ref[...], raw_ref[p], NN).astype(BF).reshape(
            groups, depth, cols
        )
        total += dot(raw_ref[p], block_rows(w_ref, 0, p, depth), NT)
        bias_ref[p : p + 1] = column_sum(raw_ref[p].astype(F32))
    out_ref[:, 0, 3 * depth :] = dot(attn_t_ref[...], ctx_ref[...], NN).astype(BF).reshape(
        groups, depth, cols
    )
    sum_ref[...] = total

    @pl.when(step == pl.num_programs(0) - 1)
    def _():
        rows_ref[...] = sum_ref[...].astype(BF)


def attn_weights(x, grad_attn, context, grad_raw, attn_w, grad_first):
    rows, features = x.shape
    groups, members, depth4, cols = attn_w.shape

    def fixed(n):
        return pl.BlockSpec((rows, n), lambda t: (0, 0), pipeline_mode=pl.Buffered(1))

    return pl.pallas_call(
        attn_weights_kernel,
        grid=(members,),
        in_specs=[
            fixed(features), fixed(features), pl.BlockSpec((rows, cols), lambda t: (0, t)),
            pl.BlockSpec((3, rows, cols), lambda t: (0, 0, t)),
            pl.BlockSpec((groups, 1, depth4, cols), lambda t: (0, t, 0, 0)), fixed(features),
        ],
        out_specs=[
            pl.BlockSpec((groups, 1, depth4, cols), lambda t: (0, t, 0, 0)),
            pl.BlockSpec((rows, features), lambda t: (0, 0)),
            pl.BlockSpec((8, cols), lambda t: (0, t)),
        ],
        out_shape=[
            jax.ShapeDtypeStruct((groups, members, depth4, cols), BF),
            jax.ShapeDtypeStruct((rows, features), BF),
            jax.ShapeDtypeStruct((8, features), F32),
        ],
        scratch_shapes=[
            pltpu.VMEM((features, rows), BF), pltpu.VMEM((features, rows), BF),
            pltpu.VMEM((rows, features), F32),
        ],
        compiler_params=pltpu.CompilerParams(vmem_limit_bytes=VMEM_BYTES),
        name="attn_weights",
    )(x, grad_attn, context, grad_raw, attn_w, grad_first)


def merge_groups(w, parts):
    groups, members, rows, cols = w.shape
    depth = rows // parts
    if depth % 16 == 0:
        return w
    w = w.reshape(groups, members, parts, depth, cols).transpose(1, 2, 0, 3, 4)
    return w.reshape(1, members, parts * groups * depth, cols)


def split_groups(w, parts, groups):
    have, members, rows, cols = w.shape
    if have == groups:
        return w
    w = w.reshape(members, parts, groups, rows // parts // groups, cols).transpose(2, 0, 1, 3, 4)
    return w.reshape(groups, members, rows // groups, cols)


def layer(rows, cotangent, bias, cos_table, sine_table, attn_w, ffn_w, b_qkv, b_up, vectors):
    qkv = project(rows, attn_w, b_qkv[:, None, :], cos_table, sine_table)
    context, lse = attend(qkv, bias)
    mixed, act, g_up, mid, g_down, g_attn, g_first, g_ctx, small, small_up = middle(
        rows, context, cotangent, bias, attn_w, ffn_w, vectors, b_up
    )
    g_ffn = ffn_weights(mid, g_down, act, g_up, ffn_w.shape[0], ffn_w.shape[1])
    g_raw = attend_back(qkv, bias, context, g_ctx, lse, cos_table, sine_table)
    g_attn_w, grad_rows, small_qkv = attn_weights(rows, g_attn, context, g_raw, attn_w, g_first)
    packed = jnp.concatenate([small_qkv[:3], small[1:7], small_up.reshape(-1, small.shape[1])], axis=0)
    return mixed, grad_rows, g_attn_w, g_ffn, packed


MESH = pl.DeviceIdType.MESH


def axis_orders(bits, rows):
    core = bits - 2
    rest = [d for d in range(bits) if d != core]
    if bits != 5 or rows % 192:
        return [(0, rows, tuple(rest) + (core,))]
    far, near, y, _, x = range(5)
    unit = rows // 12
    return [
        (0, 5 * unit, (far, near, x, y, core)),
        (5 * unit, 5 * unit, (far, near, y, x, core)),
        (10 * unit, 2 * unit, (x, y, near, far, core)),
    ]


class Place:
    def __init__(self, devices, members):
        self.devices, self.members = devices, members
        self.bits = devices.bit_length() - 1
        self.me = lax.axis_index("dp") * members + lax.axis_index("tensor")
        self.bit = [self.me // self.stride(d) % 2 for d in range(self.bits)]

    def stride(self, dim):
        return 1 << (self.bits - 1 - dim)

    def ident(self, number):
        return (number // self.members, number % self.members)

    def partner(self, dim):
        return self.ident(self.me + (1 - 2 * self.bit[dim]) * self.stride(dim))

    def meet_all(self):
        barrier = pltpu.get_barrier_semaphore()

        def greet(offset, carry):
            pl.semaphore_signal(
                barrier, inc=1, device_id=self.ident((self.me + offset) % self.devices),
                device_id_type=MESH,
            )
            return carry

        lax.fori_loop(1, self.devices, greet, 0)
        pl.semaphore_wait(barrier, self.devices - 1)

    def swap(self, src, dst, send_sem, recv_sem, offset):
        target = self.other(offset)
        return pltpu.make_async_remote_copy(
            src_ref=src.at[target], dst_ref=dst.at[self.me], send_sem=send_sem.at[offset],
            recv_sem=recv_sem.at[offset], device_id=self.ident(target), device_id_type=MESH,
        )

    def other(self, offset):
        planes = self.devices // 8
        return (self.me // 8 + offset // 8) % planes * 8 + (self.me + offset) % 8

    def for_others(self, action, first=1, last=None):
        def one(offset, carry):
            action(offset)
            return carry

        lax.fori_loop(first, self.devices if last is None else last, one, 0)

    def share(self, step, near_first):
        cuts = [1, 4, 8, 18, 28, 32] if near_first else [32, 24, 14, 8, 4, 1]
        if self.devices != 32:
            cuts = [1 + (self.devices - 1) * s // self.bits for s in range(self.bits + 1)]
        first, last = cuts[step], cuts[step + 1]
        return min(first, last), max(first, last)


def head_kernel(
    rows_ref, shard_ref, bias_ref, place_ref, length_ref, inverse_ref,
    seq_ref, attn_ref, biases_ref, cos_ref, sine_ref, mask_ref, held_ref, send_sem, recv_sem, w_send, w_recv, b_sem, local_sem, *, devices, members
):
    here = Place(devices, members)
    bits = here.bits
    colours = axis_orders(bits, shard_ref.shape[0])
    mine = pltpu.make_async_copy(rows_ref.at[here.me], held_ref, local_sem.at[0])
    mine.start()
    own = pltpu.make_async_copy(shard_ref, attn_ref.at[tuple(here.bit)], local_sem.at[1])
    own.start()
    own_bias = pltpu.make_async_copy(bias_ref, biases_ref.at[here.me % members], local_sem.at[2])
    own_bias.start()
    here.meet_all()

    def spread(colour, step):
        start, count, order = colours[colour]
        done = set(order[:step])
        span = pl.ds(start, count)
        place = tuple(slice(None) if d in done else here.bit[d] for d in range(bits))
        there = attn_ref.at[place + (span, slice(None))]
        return pltpu.make_async_remote_copy(
            src_ref=shard_ref.at[span] if step == 0 else there, dst_ref=there,
            send_sem=w_send.at[colour, step], recv_sem=w_recv.at[colour, step],
            device_id=here.partner(order[step]), device_id_type=MESH,
        )

    to_member = pltpu.make_async_remote_copy(
        src_ref=bias_ref, dst_ref=biases_ref.at[here.me % members], send_sem=b_sem.at[0],
        recv_sem=b_sem.at[1], device_id=here.partner(bits - 1), device_id_type=MESH,
    )
    moving = [spread(c, 0) for c in range(len(colours))]
    for copy in moving:
        copy.start()
    to_member.start()
    here.for_others(lambda o: here.swap(rows_ref, seq_ref, send_sem, recv_sem, o).start(), *here.share(0, True))
    mine.wait()
    back = pltpu.make_async_copy(held_ref, seq_ref.at[here.me], local_sem.at[0])
    back.start()
    place = place_ref[...]
    angles = place.astype(F32) * inverse_ref[...]
    cos_ref[...] = jnp.cos(angles)
    sine_ref[...] = jnp.sin(angles)
    mask_ref[...] = jnp.where(
        jnp.broadcast_to(place, mask_ref.shape) < length_ref[...], 0.0, MASK_FILL
    ).astype(BF)
    own.wait()
    own_bias.wait()
    for step in range(bits):
        for c in range(len(colours)):
            moving[c].wait()
            if step + 1 < bits:
                moving[c] = spread(c, step + 1)
                moving[c].start()
        if step + 1 < bits:
            here.for_others(
                lambda o: here.swap(rows_ref, seq_ref, send_sem, recv_sem, o).start(),
                *here.share(step + 1, True),
            )
    to_member.wait()
    back.wait()
    here.for_others(lambda o: here.swap(rows_ref, seq_ref, send_sem, recv_sem, o).wait())


def head(tokens, attn_shard, biases, order, length, members):
    devices, stripe, features = tokens.shape
    bits = devices.bit_length() - 1
    colours = len(axis_orders(bits, attn_shard.shape[0]))
    anywhere = pl.BlockSpec(memory_space=pl.ANY)
    onchip = pl.BlockSpec(memory_space=pltpu.VMEM)
    sems = pltpu.SemaphoreType.DMA
    slot = order.shape[0]
    seq, attn, both, cos_table, sine_table, mask = pl.pallas_call(
        functools.partial(head_kernel, devices=devices, members=members),
        in_specs=[anywhere] + [onchip] * 5,
        out_specs=[anywhere] * 3 + [onchip] * 3,
        out_shape=[
            jax.ShapeDtypeStruct(tokens.shape, BF),
            jax.ShapeDtypeStruct((2,) * bits + attn_shard.shape, BF),
            jax.ShapeDtypeStruct((members,) + biases.shape, F32),
            jax.ShapeDtypeStruct((slot, LANES), F32),
            jax.ShapeDtypeStruct((slot, LANES), F32),
            jax.ShapeDtypeStruct((slot, LANES), BF),
        ],
        scratch_shapes=[
            pltpu.VMEM((stripe, features), BF), sems((devices,)), sems((devices,)),
            sems((colours, bits)), sems((colours, bits)), sems((2,)), sems((3,)),
        ],
        compiler_params=pltpu.CompilerParams(collective_id=0, has_side_effects=True),
        name="head",
    )(tokens, attn_shard, biases, order[:, None], length.reshape(1, 1), inverse_steps())
    return seq, attn.reshape((devices,) + attn_shard.shape), both, cos_table, sine_table, mask


def tail_kernel(
    rows_ref, grad_ref, small_ref, back_ref, sum_ref, total_ref, held_ref, *rest, devices, members
):
    here = Place(devices, members)
    bits = here.bits
    colours = axis_orders(bits, grad_ref.shape[-2])
    count = len(colours)
    got = [rest[c * bits : (c + 1) * bits] for c in range(count)]
    kept = [rest[(count + c) * bits : (count + c + 1) * bits] for c in range(count)]
    small_got, small_kept = rest[2 * count * bits : 2 * count * bits + 2]
    send_sem, recv_sem, w_send, w_recv, s_send, s_recv, local_sem = rest[2 * count * bits + 2 :]
    mine = pltpu.make_async_copy(rows_ref.at[here.me], held_ref, local_sem.at[0])
    mine.start()
    here.meet_all()

    def current(colour, step):
        start, size, _ = colours[colour]
        if step == 0:
            return grad_ref, (pl.ds(start, size), slice(None))
        return kept[colour][step - 1], (slice(None), slice(None))

    def place(colour, step, side):
        order = colours[colour][2][::-1]
        left = [d for d in range(bits) if d not in order[:step]]
        return tuple(
            (here.bit[d] if side else 1 - here.bit[d]) if d == order[step] else slice(None)
            for d in left
        )

    def hand_over(colour, step):
        ref, inner = current(colour, step)
        return pltpu.make_async_remote_copy(
            src_ref=ref.at[place(colour, step, False) + inner], dst_ref=got[colour][step],
            send_sem=w_send.at[colour, step], recv_sem=w_recv.at[colour, step],
            device_id=here.partner(colours[colour][2][::-1][step]), device_id_type=MESH,
        )

    def hand_small(step):
        return pltpu.make_async_remote_copy(
            src_ref=small_ref if step == 0 else small_kept.at[step - 1], dst_ref=small_got.at[step],
            send_sem=s_send.at[step], recv_sem=s_recv.at[step],
            device_id=here.partner(bits - 1 - step), device_id_type=MESH,
        )

    moving = [hand_over(c, 0) for c in range(count)]
    for copy in moving:
        copy.start()
    small = hand_small(0)
    small.start()
    here.for_others(lambda o: here.swap(rows_ref, back_ref, send_sem, recv_sem, o).start(), *here.share(0, False))
    mine.wait()
    back = pltpu.make_async_copy(held_ref, back_ref.at[here.me], local_sem.at[0])
    back.start()
    for step in range(bits):
        for c in range(count):
            moving[c].wait()
            ref, inner = current(c, step)
            added = ref[place(c, step, True) + inner] + got[c][step][...]
            if step + 1 < bits:
                kept[c][step][...] = added
                moving[c] = hand_over(c, step + 1)
                moving[c].start()
            else:
                start, size, _ = colours[c]
                sum_ref[start : start + size] = added.astype(F32)
        if step + 1 < bits:
            here.for_others(
                lambda o: here.swap(rows_ref, back_ref, send_sem, recv_sem, o).start(),
                *here.share(step + 1, False),
            )
        small.wait()
        before = small_ref[...] if step == 0 else small_kept[step - 1]
        after = before + small_got[step]
        if step + 1 < bits:
            small_kept[step] = after
            small = hand_small(step + 1)
            small.start()
        else:
            total_ref[...] = after
    back.wait()
    here.for_others(lambda o: here.swap(rows_ref, back_ref, send_sem, recv_sem, o).wait())


def tail(grad_rows, grad_w, small, members):
    devices, stripe, features = grad_rows.shape
    bits = devices.bit_length() - 1
    rows, cols = grad_w.shape[1:]
    colours = axis_orders(bits, rows)
    anywhere = pl.BlockSpec(memory_space=pl.ANY)
    onchip = pl.BlockSpec(memory_space=pltpu.VMEM)
    sems = pltpu.SemaphoreType.DMA
    levels = [
        pltpu.VMEM((2,) * (bits - 1 - step) + (size, cols), BF)
        for _, size, _ in colours
        for step in range(bits)
    ]
    return pl.pallas_call(
        functools.partial(tail_kernel, devices=devices, members=members),
        in_specs=[anywhere, onchip, onchip],
        out_specs=[anywhere, onchip, onchip],
        out_shape=[
            jax.ShapeDtypeStruct(grad_rows.shape, BF),
            jax.ShapeDtypeStruct((rows, cols), F32),
            jax.ShapeDtypeStruct(small.shape, F32),
        ],
        scratch_shapes=[pltpu.VMEM((stripe, features), BF)] + levels + levels + [
            pltpu.VMEM((bits,) + small.shape, F32), pltpu.VMEM((bits,) + small.shape, F32),
            sems((devices,)), sems((devices,)), sems((len(colours), bits)), sems((len(colours), bits)),
            sems((bits,)), sems((bits,)), sems((1,)),
        ],
        compiler_params=pltpu.CompilerParams(
            collective_id=1, has_side_effects=True, vmem_limit_bytes=VMEM_BYTES
        ),
        name="tail",
    )(grad_rows, grad_w.reshape((2,) * bits + (rows, cols)), small)


def body(
    tokens, out_grad, lengths, order, w_qkv, b_qkv, w_out, b_out, norm1_gain, norm1_bias,
    w_up, b_up, w_down, b_down, norm2_gain, norm2_bias,
):
    dp_size = lax.axis_size("dp")
    tp_size = lax.axis_size("tensor")
    devices = dp_size * tp_size
    me = lax.axis_index(AXES)
    stored, stripe, features = tokens.shape
    slot = devices * stripe
    depth = w_qkv.shape[1]
    cols = w_qkv.shape[2]
    units = w_up.shape[1]

    def deal(rows_val):
        return lax.all_to_all(rows_val, AXES, split_axis=0, concat_axis=0, tiled=True)

    ffn_shard = jnp.concatenate([w_up, w_down.T], axis=0)
    ffn_all = lax.all_gather(ffn_shard, AXES, axis=0, tiled=True)
    ffn_w = merge_groups(ffn_all.reshape(dp_size, tp_size, 2 * depth, units), 2)
    attn_shard = jnp.concatenate([w_qkv.reshape(3 * depth, cols), w_out.T], axis=0)
    biases = jnp.concatenate([b_qkv.reshape(-1), b_up]).reshape(-1, LANES)
    length = lax.dynamic_index_in_dim(lengths, me, 0, keepdims=False)
    rows, attn_all, biases, cos_table, sine_table, mask = head(
        tokens, attn_shard, biases, order, length, tp_size
    )
    rows = rows.reshape(slot, features)
    attn_w = merge_groups(attn_all.reshape(dp_size, tp_size, 4 * depth, cols), 4)
    biases = biases.reshape(tp_size, -1)
    b_qkv_all = biases[:, : 3 * cols].reshape(tp_size, 3, cols).transpose(1, 0, 2).reshape(3, features)
    b_up_all = biases[:, 3 * cols :].reshape(1, tp_size * units)
    rows, out_grad = lax.optimization_barrier((rows, out_grad))
    cotangent = deal(out_grad).reshape(slot, features)
    none = jnp.zeros_like(b_out)
    vectors = jnp.stack(
        [b_out, norm1_gain, norm1_bias, b_down, norm2_gain, norm2_bias, none, none], axis=0
    )
    result, grad_rows, g_attn_w, g_ffn, packed = layer(
        rows, cotangent, mask, cos_table, sine_table, attn_w, ffn_w, b_qkv_all, b_up_all, vectors
    )
    mixed = deal(result.reshape(devices, stripe, features))
    laid = split_groups(g_ffn, 2, dp_size).reshape(devices * 2 * depth, units)
    ffn_sum = lax.psum_scatter(laid, AXES, scatter_dimension=0, tiled=True).astype(F32)
    laid = split_groups(g_attn_w, 4, dp_size).reshape(devices, 4 * depth, cols)
    packed = jnp.pad(packed, ((0, -packed.shape[0] % 8), (0, 0)))
    grad_tokens, attn_sum, summed = tail(
        grad_rows.reshape(devices, stripe, features), laid, packed, tp_size
    )
    return (
        mixed, grad_tokens, attn_sum[: 3 * depth].reshape(3, depth, cols), summed[:3],
        attn_sum[3 * depth :].T, summed[3], summed[4], summed[5], ffn_sum[:depth],
        summed[9:13].reshape(-1), ffn_sum[depth:].T, summed[6], summed[7], summed[8],
    )


def solution(mesh):
    rows = P(None, AXES, None)
    in_specs = (
        rows, rows, P(), P(), P(None, "dp", "tensor"), P(None, "tensor"), P("tensor", "dp"), P(),
        P(), P(), P("dp", "tensor"), P("tensor"), P("tensor", "dp"), P(), P(), P(),
    )
    out_specs = (
        rows, rows, P(None, "dp", "tensor"), P(), P("tensor", "dp"), P(), P(), P(),
        P("dp", "tensor"), P(), P("tensor", "dp"), P(), P(), P(),
    )
    return jax.shard_map(body, mesh=mesh, in_specs=in_specs, out_specs=out_specs, check_vma=False)
```

```python
import functools

import jax
import jax.numpy as jnp
from jax import lax
from jax.experimental import pallas as pl
from jax.experimental.pallas import tpu as pltpu
from jax.sharding import PartitionSpec as P

HD = 64
LANES = 128
NORM_EPS = 1e-12
ROPE_BASE = 10000.0
MASK_FILL = -1e30
SCORE_SCALE = 0.125
INV_ROOT_TWO = 0.7071067811865476
INV_ROOT_TAU = 0.3989422804014327
AXES = ("dp", "tensor")
BF = jnp.bfloat16
F32 = jnp.float32
VMEM_BYTES = 60 * 1024 * 1024
VMEM_LESS = 32 * 1024 * 1024


def dot(a, b, dims):
    return lax.dot_general(a, b, (dims, ((), ())), preferred_element_type=F32)


NN = ((1,), (0,))
NT = ((1,), (1,))
TN = ((0,), (0,))


def inverse_steps():
    steps = (jnp.arange(LANES) % HD // 2).astype(F32)
    return jnp.power(ROPE_BASE, -2.0 * steps / HD)[None, :]


def turn(values, cos_table, sine_table):
    lane = lax.broadcasted_iota(jnp.int32, values.shape, 1)
    swapped = jnp.where(
        lane % 2 == 0, -pltpu.roll(values, LANES - 1, 1), pltpu.roll(values, 1, 1)
    )
    return values * cos_table + swapped * sine_table


def block_rows(w_ref, member, part, depth, cols=slice(None)):
    taken = w_ref[:, member, part * depth : (part + 1) * depth, cols]
    return taken.reshape(taken.shape[0] * depth, taken.shape[2])


def project_kernel(x_ref, w_ref, b_ref, cos_ref, sine_ref, out_ref):
    kind = pl.program_id(0)
    depth = w_ref.shape[2]
    weight = [block_rows(w_ref, t, 0, depth) for t in range(w_ref.shape[1])]
    raw = dot(x_ref[...], jnp.concatenate(weight, axis=1), NN) + b_ref[0]

    @pl.when(kind < 2)
    def _():
        for part in range(raw.shape[1] // LANES):
            cols = slice(part * LANES, (part + 1) * LANES)
            out_ref[0, :, cols] = turn(raw[:, cols], cos_ref[...], sine_ref[...]).astype(BF)

    @pl.when(kind == 2)
    def _():
        out_ref[0] = raw.astype(BF)


def project(x, attn_w, b, cos_table, sine_table):
    rows, features = x.shape
    groups, members, depth4, cols = attn_w.shape
    depth = depth4 // 4
    tile = rows
    return pl.pallas_call(
        project_kernel,
        grid=(3, rows // tile),
        in_specs=[
            pl.BlockSpec((tile, features), lambda p, r: (r, 0)),
            pl.BlockSpec((groups, members, depth, cols), lambda p, r: (0, 0, p, 0)),
            pl.BlockSpec((1, 1, features), lambda p, r: (p, 0, 0)),
            pl.BlockSpec((tile, LANES), lambda p, r: (r, 0)),
            pl.BlockSpec((tile, LANES), lambda p, r: (r, 0)),
        ],
        out_specs=pl.BlockSpec((1, tile, features), lambda p, r: (p, r, 0)),
        out_shape=jax.ShapeDtypeStruct((3, rows, features), BF),
        compiler_params=pltpu.CompilerParams(vmem_limit_bytes=VMEM_LESS),
        name="project",
    )(x, attn_w, b, cos_table, sine_table)


def pair_operands(q, k, bias, lane, head):
    inside = lane // HD == head
    spare = lane == (1 - head) * HD
    zero = jnp.zeros_like(q)
    q_head = jnp.where(inside, q, jnp.where(spare, jnp.ones_like(q), zero))
    k_head = jnp.where(inside, k, jnp.where(spare, bias, zero))
    return q_head, k_head


def attend_kernel(q_ref, k_ref, v_ref, bias_ref, ctx_ref, lse_ref, *, chunk):
    rows = q_ref.shape[1]
    lane = lax.broadcasted_iota(jnp.int32, (rows, LANES), 1)
    q = q_ref[0] * jnp.asarray(SCORE_SCALE, BF)
    k = k_ref[0]
    v_turned = v_ref[0].T
    ones = jnp.ones((16, rows), BF)
    v_heads = [
        jnp.concatenate([v_turned[head * HD : (head + 1) * HD], ones], axis=0) for head in range(2)
    ]
    bias = bias_ref[...]
    for part in range(rows // chunk):
        span = slice(part * chunk, (part + 1) * chunk)
        outs = []
        for head in range(2):
            q_head, k_head = pair_operands(q, k, bias, lane, head)
            scores = dot(k_head, q_head[span], NT)
            tops = jnp.max(scores.reshape(16, rows // 16, chunk), axis=0)
            top = jnp.max(tops, axis=0, keepdims=True)
            expo = jnp.exp(scores - top)
            mixed = dot(v_heads[head], expo.astype(BF), NN)
            total = mixed[HD : HD + 1]
            outs.append(mixed[:HD] / total)
            lse_ref[0, head : head + 1, span] = top + jnp.log(total)
        ctx_ref[span, :] = jnp.concatenate(outs, axis=0).T.astype(BF)


def attend(qkv, bias):
    _, rows, features = qkv.shape
    pairs = features // LANES
    chunk = rows

    def spec(which):
        return pl.BlockSpec((1, rows, LANES), lambda h: (which, 0, h))

    return pl.pallas_call(
        functools.partial(attend_kernel, chunk=chunk),
        grid=(pairs,),
        in_specs=[spec(0), spec(1), spec(2), pl.BlockSpec((rows, LANES), lambda h: (0, 0))],
        out_specs=[
            pl.BlockSpec((rows, LANES), lambda h: (0, h)),
            pl.BlockSpec((1, 2, rows), lambda h: (h, 0, 0)),
        ],
        out_shape=[
            jax.ShapeDtypeStruct((rows, features), BF),
            jax.ShapeDtypeStruct((pairs, 2, rows), F32),
        ],
        compiler_params=pltpu.CompilerParams(vmem_limit_bytes=VMEM_LESS),
        name="attend",
    )(qkv, qkv, qkv, bias)


def attend_back_kernel(
    q_ref, k_ref, v_ref, bias_ref, ctx_ref, grad_ref, lse_ref, cos_ref, sine_ref, out_ref,
    dk_ref, dv_ref, *, chunk
):
    rows = q_ref.shape[1]
    lane = lax.broadcasted_iota(jnp.int32, (rows, LANES), 1)
    q = q_ref[0] * jnp.asarray(SCORE_SCALE, BF)
    k = k_ref[0]
    v = v_ref[0]
    grad = grad_ref[...]
    bias = bias_ref[...]
    k_turned = k.T
    zero = jnp.zeros_like(grad)
    dots = (grad.astype(F32) * ctx_ref[...].astype(F32)).T
    for part in range(rows // chunk):
        span = slice(part * chunk, (part + 1) * chunk)
        dq_parts = []
        dk_sum = None
        dv_sum = None
        for head in range(2):
            q_head, k_head = pair_operands(q, k, bias, lane, head)
            inside = lane // HD == head
            g_head = jnp.where(inside, grad, zero)[span]
            q_only = jnp.where(inside, q, zero)[span]
            scores = dot(k_head, q_head[span], NT)
            prob = jnp.exp(scores - lse_ref[0, head : head + 1, span])
            g_prob = dot(v, g_head, NT)
            inner = jnp.sum(dots[head * HD : (head + 1) * HD, span], axis=0, keepdims=True)
            g_score = (prob * (g_prob - inner)).astype(BF)
            dv = dot(prob.astype(BF), g_head, NN)
            dk = dot(g_score, q_only, NN)
            dq_parts.append(dot(k_turned[head * HD : (head + 1) * HD], g_score, NN))
            dk_sum = dk if dk_sum is None else dk_sum + dk
            dv_sum = dv if dv_sum is None else dv_sum + dv
        dq = jnp.concatenate(dq_parts, axis=0).T * SCORE_SCALE
        out_ref[0, span, :] = turn(dq, cos_ref[span, :], -sine_ref[span, :]).astype(BF)
        if part == 0:
            dk_ref[...] = dk_sum
            dv_ref[...] = dv_sum
        else:
            dk_ref[...] += dk_sum
            dv_ref[...] += dv_sum
    out_ref[1] = turn(dk_ref[...], cos_ref[...], -sine_ref[...]).astype(BF)
    out_ref[2] = dv_ref[...].astype(BF)


def attend_back(qkv, bias, context, grad_ctx, lse, cos_table, sine_table):
    _, rows, features = qkv.shape
    pairs = features // LANES
    chunk = 256

    def spec(which):
        return pl.BlockSpec((1, rows, LANES), lambda h: (which, 0, h))

    fixed = pl.BlockSpec((rows, LANES), lambda h: (0, 0))
    cols = pl.BlockSpec((rows, LANES), lambda h: (0, h))
    return pl.pallas_call(
        functools.partial(attend_back_kernel, chunk=chunk),
        grid=(pairs,),
        in_specs=[
            spec(0), spec(1), spec(2), fixed, cols, cols,
            pl.BlockSpec((1, 2, rows), lambda h: (h, 0, 0)), fixed, fixed,
        ],
        out_specs=pl.BlockSpec((3, rows, LANES), lambda h: (0, 0, h)),
        out_shape=jax.ShapeDtypeStruct((3, rows, features), BF),
        scratch_shapes=[pltpu.VMEM((rows, LANES), F32), pltpu.VMEM((rows, LANES), F32)],
        compiler_params=pltpu.CompilerParams(vmem_limit_bytes=VMEM_BYTES),
        name="attend_back",
    )(qkv, qkv, qkv, bias, context, grad_ctx, lse, cos_table, sine_table)


def normalize(hidden, gain_vec, shift_vec):
    row_mean = jnp.mean(hidden, axis=-1, keepdims=True)
    centred = hidden - row_mean
    row_var = jnp.mean(centred * centred, axis=-1, keepdims=True)
    inv_std = lax.rsqrt(row_var + NORM_EPS)
    normed = centred * inv_std
    return (normed * gain_vec + shift_vec, normed, inv_std)


def normalize_back(grad_unit, normed, inv_std):
    first_mean = jnp.mean(grad_unit, axis=-1, keepdims=True)
    second_mean = jnp.mean(grad_unit * normed, axis=-1, keepdims=True)
    return inv_std * (grad_unit - first_mean - normed * second_mean)


def column_sum(values):
    rows = values.shape[0]
    grouped = jnp.sum(values.reshape(rows // 32, 32, values.shape[1]), axis=0)
    return jnp.sum(grouped, axis=0, keepdims=True)


def middle_kernel(
    x_ref, ctx_ref, cot_ref, live_ref, attn_ref, ffn_ref, vec_ref, b_up_ref,
    mixed_ref, act_ref, g_up_ref, mid_ref, g_down_ref, g_attn_ref, g_first_ref, g_ctx_ref,
    small_ref, small_up_ref, slope_ref, *, chunk
):
    members, depth, cols = attn_ref.shape[1], attn_ref.shape[2], attn_ref.shape[3]
    ffn_depth, units = ffn_ref.shape[2] // 2, ffn_ref.shape[3]
    b_out, gain_one, shift_one = vec_ref[0:1], vec_ref[1:2], vec_ref[2:3]
    b_down, gain_two, shift_two = vec_ref[3:4], vec_ref[4:5], vec_ref[5:6]

    @pl.when(pl.program_id(0) == 0)
    def _():
        small_ref[...] = jnp.zeros_like(small_ref)
        small_up_ref[...] = jnp.zeros_like(small_up_ref)

    first_sum = x_ref[...].astype(F32) + b_out
    for t in range(members):
        first_sum += dot(ctx_ref[:, t * cols : (t + 1) * cols], block_rows(attn_ref, t, 0, depth), NT)
    normed_one, unit_one, inv_one = normalize(first_sum, gain_one, shift_one)
    mid = normed_one.astype(BF)
    mid_ref[...] = mid
    second_sum = normed_one + b_down
    for t in range(members):
        for start in range(0, units, chunk):
            here = slice(t * units + start, t * units + start + chunk)
            span = slice(start, start + chunk)
            up_proj = dot(mid, block_rows(ffn_ref, t, 0, ffn_depth, span), NN) + b_up_ref[:, here]
            phi = 0.5 * (1.0 + lax.erf(up_proj * INV_ROOT_TWO))
            act_ref[:, here] = (up_proj * phi).astype(BF)
            slope_ref[:, here] = phi + up_proj * jnp.exp(-0.5 * up_proj * up_proj) * INV_ROOT_TAU
        half = slice(t * units, (t + 1) * units)
        second_sum += dot(act_ref[:, half], block_rows(ffn_ref, t, 1, ffn_depth), NT)
    result, unit_two, inv_two = normalize(second_sum, gain_two, shift_two)
    mixed_ref[...] = result.astype(BF)

    grad_out = jnp.where(live_ref[:, 0:1].astype(F32) == 0.0, cot_ref[...].astype(F32), 0.0)
    grad_second = normalize_back(grad_out * gain_two, unit_two, inv_two)
    small_ref[5:6] += column_sum(grad_out * unit_two)
    small_ref[6:7] += column_sum(grad_out)
    small_ref[4:5] += column_sum(grad_second)
    grad_down = grad_second.astype(BF)
    g_down_ref[...] = grad_down
    grad_mid = grad_second
    for t in range(members):
        for start in range(0, units, chunk):
            here = slice(t * units + start, t * units + start + chunk)
            span = slice(start, start + chunk)
            grad_act = dot(grad_down, block_rows(ffn_ref, t, 1, ffn_depth, span), NN)
            grad_up = (grad_act * slope_ref[:, here]).astype(BF)
            g_up_ref[:, here] = grad_up
            small_up_ref[:, here] += column_sum(grad_up.astype(F32))
        half = slice(t * units, (t + 1) * units)
        grad_mid += dot(g_up_ref[:, half], block_rows(ffn_ref, t, 0, ffn_depth), NT)
    small_ref[2:3] += column_sum(grad_mid * unit_one)
    small_ref[3:4] += column_sum(grad_mid)
    grad_first = normalize_back(grad_mid * gain_one, unit_one, inv_one)
    small_ref[1:2] += column_sum(grad_first)
    g_first_ref[...] = grad_first
    grad_attn = grad_first.astype(BF)
    g_attn_ref[...] = grad_attn
    for t in range(members):
        g_ctx_ref[:, t * cols : (t + 1) * cols] = dot(
            grad_attn, block_rows(attn_ref, t, 0, depth), NN
        ).astype(BF)


def middle(x, context, cotangent, live, attn_w, ffn_w, vectors, b_up):
    rows, features = x.shape
    groups, members, depth4, cols = attn_w.shape
    ffn_rows, units = ffn_w.shape[2], ffn_w.shape[3]
    width = members * units
    tile = 256

    def row(n):
        return pl.BlockSpec((tile, n), lambda i: (i, 0))

    def fixed(shape, index):
        return pl.BlockSpec(shape, lambda i: index, pipeline_mode=pl.Buffered(1))

    def out(n, dtype):
        return jax.ShapeDtypeStruct((rows, n), dtype)

    return pl.pallas_call(
        functools.partial(middle_kernel, chunk=512),
        grid=(rows // tile,),
        in_specs=[
            row(features), row(features), row(features), row(LANES),
            fixed((groups, members, depth4 // 4, cols), (0, 0, 3, 0)),
            fixed((groups, members, ffn_rows, units), (0, 0, 0, 0)),
            fixed((8, features), (0, 0)), fixed((1, width), (0, 0)),
        ],
        out_specs=[
            row(features), row(width), row(width), row(features), row(features), row(features),
            row(features), row(features),
            pl.BlockSpec((8, features), lambda i: (0, 0)), pl.BlockSpec((1, width), lambda i: (0, 0)),
        ],
        out_shape=[
            out(features, BF), out(width, BF), out(width, BF), out(features, BF), out(features, BF),
            out(features, BF), out(features, F32), out(features, BF),
            jax.ShapeDtypeStruct((8, features), F32), jax.ShapeDtypeStruct((1, width), F32),
        ],
        scratch_shapes=[pltpu.VMEM((tile, width), F32)],
        compiler_params=pltpu.CompilerParams(vmem_limit_bytes=VMEM_BYTES),
        name="middle",
    )(x, context, cotangent, live, attn_w, ffn_w, vectors, b_up)


def ffn_weights_kernel(mid_ref, g_down_ref, act_ref, g_up_ref, out_ref, mid_t_ref, down_t_ref):
    groups, _, depth2, width = out_ref.shape
    depth = depth2 // 2

    @pl.when((pl.program_id(0) == 0) & (pl.program_id(1) == 0))
    def _():
        mid_t_ref[...] = mid_ref[...].T
        down_t_ref[...] = g_down_ref[...].T

    out_ref[:, 0, :depth] = dot(mid_t_ref[...], g_up_ref[...], NN).astype(BF).reshape(groups, depth, width)
    out_ref[:, 0, depth:] = dot(down_t_ref[...], act_ref[...], NN).astype(BF).reshape(groups, depth, width)


def ffn_weights(mid, grad_down, act, grad_up, groups, members):
    rows, features = mid.shape
    units = act.shape[1] // members
    chunk = 768
    per = units // chunk
    fixed = pl.BlockSpec((rows, features), lambda t, j: (0, 0), pipeline_mode=pl.Buffered(1))
    part = pl.BlockSpec((rows, chunk), lambda t, j: (0, t * per + j))
    depth2 = 2 * features // groups
    return pl.pallas_call(
        ffn_weights_kernel,
        grid=(members, per),
        in_specs=[fixed, fixed, part, part],
        out_specs=pl.BlockSpec((groups, 1, depth2, chunk), lambda t, j: (0, t, 0, j)),
        out_shape=jax.ShapeDtypeStruct((groups, members, depth2, units), BF),
        scratch_shapes=[pltpu.VMEM((features, rows), BF), pltpu.VMEM((features, rows), BF)],
        compiler_params=pltpu.CompilerParams(vmem_limit_bytes=VMEM_BYTES),
        name="ffn_weights",
    )(mid, grad_down, act, grad_up)


def attn_weights_kernel(
    x_ref, g_attn_ref, ctx_ref, raw_ref, w_ref, g_first_ref, out_ref, rows_ref, bias_ref,
    x_t_ref, attn_t_ref, sum_ref
):
    groups, _, depth4, cols = out_ref.shape
    depth = depth4 // 4
    step = pl.program_id(0)

    @pl.when(step == 0)
    def _():
        x_t_ref[...] = x_ref[...].T
        attn_t_ref[...] = g_attn_ref[...].T
        sum_ref[...] = g_first_ref[...]
        bias_ref[...] = jnp.zeros_like(bias_ref)

    total = sum_ref[...]
    for p in range(3):
        out_ref[:, 0, p * depth : (p + 1) * depth] = dot(x_t_ref[...], raw_ref[p], NN).astype(BF).reshape(
            groups, depth, cols
        )
        total += dot(raw_ref[p], block_rows(w_ref, 0, p, depth), NT)
        bias_ref[p : p + 1] = column_sum(raw_ref[p].astype(F32))
    out_ref[:, 0, 3 * depth :] = dot(attn_t_ref[...], ctx_ref[...], NN).astype(BF).reshape(
        groups, depth, cols
    )
    sum_ref[...] = total

    @pl.when(step == pl.num_programs(0) - 1)
    def _():
        rows_ref[...] = sum_ref[...].astype(BF)


def attn_weights(x, grad_attn, context, grad_raw, attn_w, grad_first):
    rows, features = x.shape
    groups, members, depth4, cols = attn_w.shape

    def fixed(n):
        return pl.BlockSpec((rows, n), lambda t: (0, 0), pipeline_mode=pl.Buffered(1))

    return pl.pallas_call(
        attn_weights_kernel,
        grid=(members,),
        in_specs=[
            fixed(features), fixed(features), pl.BlockSpec((rows, cols), lambda t: (0, t)),
            pl.BlockSpec((3, rows, cols), lambda t: (0, 0, t)),
            pl.BlockSpec((groups, 1, depth4, cols), lambda t: (0, t, 0, 0)), fixed(features),
        ],
        out_specs=[
            pl.BlockSpec((groups, 1, depth4, cols), lambda t: (0, t, 0, 0)),
            pl.BlockSpec((rows, features), lambda t: (0, 0)),
            pl.BlockSpec((8, cols), lambda t: (0, t)),
        ],
        out_shape=[
            jax.ShapeDtypeStruct((groups, members, depth4, cols), BF),
            jax.ShapeDtypeStruct((rows, features), BF),
            jax.ShapeDtypeStruct((8, features), F32),
        ],
        scratch_shapes=[
            pltpu.VMEM((features, rows), BF), pltpu.VMEM((features, rows), BF),
            pltpu.VMEM((rows, features), F32),
        ],
        compiler_params=pltpu.CompilerParams(vmem_limit_bytes=VMEM_BYTES),
        name="attn_weights",
    )(x, grad_attn, context, grad_raw, attn_w, grad_first)


def merge_groups(w, parts):
    groups, members, rows, cols = w.shape
    depth = rows // parts
    if depth % 16 == 0:
        return w
    w = w.reshape(groups, members, parts, depth, cols).transpose(1, 2, 0, 3, 4)
    return w.reshape(1, members, parts * groups * depth, cols)


def split_groups(w, parts, groups):
    have, members, rows, cols = w.shape
    if have == groups:
        return w
    w = w.reshape(members, parts, groups, rows // parts // groups, cols).transpose(2, 0, 1, 3, 4)
    return w.reshape(groups, members, rows // groups, cols)


def layer(rows, cotangent, bias, cos_table, sine_table, attn_w, ffn_w, b_qkv, b_up, vectors):
    qkv = project(rows, attn_w, b_qkv[:, None, :], cos_table, sine_table)
    context, lse = attend(qkv, bias)
    mixed, act, g_up, mid, g_down, g_attn, g_first, g_ctx, small, small_up = middle(
        rows, context, cotangent, bias, attn_w, ffn_w, vectors, b_up
    )
    g_ffn = ffn_weights(mid, g_down, act, g_up, ffn_w.shape[0], ffn_w.shape[1])
    g_raw = attend_back(qkv, bias, context, g_ctx, lse, cos_table, sine_table)
    g_attn_w, grad_rows, small_qkv = attn_weights(rows, g_attn, context, g_raw, attn_w, g_first)
    packed = jnp.concatenate([small_qkv[:3], small[1:7], small_up.reshape(-1, small.shape[1])], axis=0)
    return mixed, grad_rows, g_attn_w, g_ffn, packed


MESH = pl.DeviceIdType.MESH


def axis_orders(bits, rows):
    core = bits - 2
    rest = [d for d in range(bits) if d != core]
    if bits != 5 or rows % 192:
        return [(0, rows, tuple(rest) + (core,))]
    far, near, y, _, x = range(5)
    unit = rows // 12
    return [
        (0, 5 * unit, (far, near, x, y, core)),
        (5 * unit, 5 * unit, (far, near, y, x, core)),
        (10 * unit, 2 * unit, (x, y, near, far, core)),
    ]


class Place:
    def __init__(self, devices, members):
        self.devices, self.members = devices, members
        self.bits = devices.bit_length() - 1
        self.me = lax.axis_index("dp") * members + lax.axis_index("tensor")
        self.bit = [self.me // self.stride(d) % 2 for d in range(self.bits)]

    def stride(self, dim):
        return 1 << (self.bits - 1 - dim)

    def ident(self, number):
        return (number // self.members, number % self.members)

    def partner(self, dim):
        return self.ident(self.me + (1 - 2 * self.bit[dim]) * self.stride(dim))

    def meet_all(self):
        barrier = pltpu.get_barrier_semaphore()

        def greet(offset, carry):
            pl.semaphore_signal(
                barrier, inc=1, device_id=self.ident((self.me + offset) % self.devices),
                device_id_type=MESH,
            )
            return carry

        lax.fori_loop(1, self.devices, greet, 0)
        pl.semaphore_wait(barrier, self.devices - 1)

    def swap(self, src, dst, send_sem, recv_sem, offset):
        target = self.other(offset)
        return pltpu.make_async_remote_copy(
            src_ref=src.at[target], dst_ref=dst.at[self.me], send_sem=send_sem.at[offset],
            recv_sem=recv_sem.at[offset], device_id=self.ident(target), device_id_type=MESH,
        )

    def other(self, offset):
        planes = self.devices // 8
        return (self.me // 8 + offset // 8) % planes * 8 + (self.me + offset) % 8

    def for_others(self, action, first=1, last=None):
        def one(offset, carry):
            action(offset)
            return carry

        lax.fori_loop(first, self.devices if last is None else last, one, 0)

    def share(self, step, near_first):
        cuts = [1, 4, 8, 18, 28, 32] if near_first else [32, 24, 14, 8, 4, 1]
        if self.devices != 32:
            cuts = [1 + (self.devices - 1) * s // self.bits for s in range(self.bits + 1)]
        first, last = cuts[step], cuts[step + 1]
        return min(first, last), max(first, last)


def head_kernel(
    rows_ref, shard_ref, bias_ref, place_ref, length_ref, inverse_ref,
    seq_ref, attn_ref, biases_ref, cos_ref, sine_ref, mask_ref, held_ref, send_sem, recv_sem, w_send, w_recv, b_sem, local_sem, *, devices, members
):
    here = Place(devices, members)
    bits = here.bits
    colours = axis_orders(bits, shard_ref.shape[0])
    mine = pltpu.make_async_copy(rows_ref.at[here.me], held_ref, local_sem.at[0])
    mine.start()
    own = pltpu.make_async_copy(shard_ref, attn_ref.at[tuple(here.bit)], local_sem.at[1])
    own.start()
    own_bias = pltpu.make_async_copy(bias_ref, biases_ref.at[here.me % members], local_sem.at[2])
    own_bias.start()
    here.meet_all()

    def spread(colour, step):
        start, count, order = colours[colour]
        done = set(order[:step])
        span = pl.ds(start, count)
        place = tuple(slice(None) if d in done else here.bit[d] for d in range(bits))
        there = attn_ref.at[place + (span, slice(None))]
        return pltpu.make_async_remote_copy(
            src_ref=shard_ref.at[span] if step == 0 else there, dst_ref=there,
            send_sem=w_send.at[colour, step], recv_sem=w_recv.at[colour, step],
            device_id=here.partner(order[step]), device_id_type=MESH,
        )

    to_member = pltpu.make_async_remote_copy(
        src_ref=bias_ref, dst_ref=biases_ref.at[here.me % members], send_sem=b_sem.at[0],
        recv_sem=b_sem.at[1], device_id=here.partner(bits - 1), device_id_type=MESH,
    )
    moving = [spread(c, 0) for c in range(len(colours))]
    for copy in moving:
        copy.start()
    to_member.start()
    here.for_others(lambda o: here.swap(rows_ref, seq_ref, send_sem, recv_sem, o).start(), *here.share(0, True))
    mine.wait()
    back = pltpu.make_async_copy(held_ref, seq_ref.at[here.me], local_sem.at[0])
    back.start()
    place = jnp.broadcast_to(place_ref[...].astype(F32), (LANES, place_ref.shape[1])).T
    angles = place * inverse_ref[...]
    cos_ref[...] = jnp.cos(angles)
    sine_ref[...] = jnp.sin(angles)
    lengths = length_ref[...].astype(F32)
    ours = lax.broadcasted_iota(jnp.int32, lengths.shape, 1) == here.me
    length = jnp.sum(jnp.where(ours, lengths, 0.0), axis=1, keepdims=True)
    mask_ref[...] = jnp.where(place < length, 0.0, MASK_FILL).astype(BF)
    own.wait()
    own_bias.wait()
    for step in range(bits):
        for c in range(len(colours)):
            moving[c].wait()
            if step + 1 < bits:
                moving[c] = spread(c, step + 1)
                moving[c].start()
        if step + 1 < bits:
            here.for_others(
                lambda o: here.swap(rows_ref, seq_ref, send_sem, recv_sem, o).start(),
                *here.share(step + 1, True),
            )
    to_member.wait()
    back.wait()
    here.for_others(lambda o: here.swap(rows_ref, seq_ref, send_sem, recv_sem, o).wait())


def head(tokens, attn_shard, biases, order, lengths, members):
    devices, stripe, features = tokens.shape
    bits = devices.bit_length() - 1
    colours = len(axis_orders(bits, attn_shard.shape[0]))
    anywhere = pl.BlockSpec(memory_space=pl.ANY)
    onchip = pl.BlockSpec(memory_space=pltpu.VMEM)
    sems = pltpu.SemaphoreType.DMA
    slot = order.shape[0]
    seq, attn, both, cos_table, sine_table, mask = pl.pallas_call(
        functools.partial(head_kernel, devices=devices, members=members),
        in_specs=[anywhere] + [onchip] * 5,
        out_specs=[anywhere] * 3 + [onchip] * 3,
        out_shape=[
            jax.ShapeDtypeStruct(tokens.shape, BF),
            jax.ShapeDtypeStruct((2,) * bits + attn_shard.shape, BF),
            jax.ShapeDtypeStruct((members,) + biases.shape, F32),
            jax.ShapeDtypeStruct((slot, LANES), F32),
            jax.ShapeDtypeStruct((slot, LANES), F32),
            jax.ShapeDtypeStruct((slot, LANES), BF),
        ],
        scratch_shapes=[
            pltpu.VMEM((stripe, features), BF), sems((devices,)), sems((devices,)),
            sems((colours, bits)), sems((colours, bits)), sems((2,)), sems((3,)),
        ],
        compiler_params=pltpu.CompilerParams(collective_id=0, has_side_effects=True),
        name="head",
    )(tokens, attn_shard, biases, order[None, :], lengths[None, :], inverse_steps())
    return seq, attn.reshape((devices,) + attn_shard.shape), both, cos_table, sine_table, mask


def tail_kernel(
    rows_ref, grad_ref, small_ref, back_ref, sum_ref, total_ref, held_ref, *rest, devices, members
):
    here = Place(devices, members)
    bits = here.bits
    colours = axis_orders(bits, grad_ref.shape[-2])
    count = len(colours)
    got = [rest[c * bits : (c + 1) * bits] for c in range(count)]
    kept = [rest[(count + c) * bits : (count + c + 1) * bits] for c in range(count)]
    small_got, small_kept = rest[2 * count * bits : 2 * count * bits + 2]
    send_sem, recv_sem, w_send, w_recv, s_send, s_recv, local_sem = rest[2 * count * bits + 2 :]
    mine = pltpu.make_async_copy(rows_ref.at[here.me], held_ref, local_sem.at[0])
    mine.start()
    here.meet_all()

    def current(colour, step):
        start, size, _ = colours[colour]
        if step == 0:
            return grad_ref, (pl.ds(start, size), slice(None))
        return kept[colour][step - 1], (slice(None), slice(None))

    def place(colour, step, side):
        order = colours[colour][2][::-1]
        left = [d for d in range(bits) if d not in order[:step]]
        return tuple(
            (here.bit[d] if side else 1 - here.bit[d]) if d == order[step] else slice(None)
            for d in left
        )

    def hand_over(colour, step):
        ref, inner = current(colour, step)
        return pltpu.make_async_remote_copy(
            src_ref=ref.at[place(colour, step, False) + inner], dst_ref=got[colour][step],
            send_sem=w_send.at[colour, step], recv_sem=w_recv.at[colour, step],
            device_id=here.partner(colours[colour][2][::-1][step]), device_id_type=MESH,
        )

    def hand_small(step):
        return pltpu.make_async_remote_copy(
            src_ref=small_ref if step == 0 else small_kept.at[step - 1], dst_ref=small_got.at[step],
            send_sem=s_send.at[step], recv_sem=s_recv.at[step],
            device_id=here.partner(bits - 1 - step), device_id_type=MESH,
        )

    moving = [hand_over(c, 0) for c in range(count)]
    for copy in moving:
        copy.start()
    small = hand_small(0)
    small.start()
    here.for_others(lambda o: here.swap(rows_ref, back_ref, send_sem, recv_sem, o).start(), *here.share(0, False))
    mine.wait()
    back = pltpu.make_async_copy(held_ref, back_ref.at[here.me], local_sem.at[0])
    back.start()
    for step in range(bits):
        for c in range(count):
            moving[c].wait()
            ref, inner = current(c, step)
            added = ref[place(c, step, True) + inner] + got[c][step][...]
            if step + 1 < bits:
                kept[c][step][...] = added
                moving[c] = hand_over(c, step + 1)
                moving[c].start()
            else:
                start, size, _ = colours[c]
                sum_ref[start : start + size] = added.astype(F32)
        if step + 1 < bits:
            here.for_others(
                lambda o: here.swap(rows_ref, back_ref, send_sem, recv_sem, o).start(),
                *here.share(step + 1, False),
            )
        small.wait()
        before = small_ref[...] if step == 0 else small_kept[step - 1]
        after = before + small_got[step]
        if step + 1 < bits:
            small_kept[step] = after
            small = hand_small(step + 1)
            small.start()
        else:
            total_ref[...] = after
    back.wait()
    here.for_others(lambda o: here.swap(rows_ref, back_ref, send_sem, recv_sem, o).wait())


def tail(grad_rows, grad_w, small, members):
    devices, stripe, features = grad_rows.shape
    bits = devices.bit_length() - 1
    rows, cols = grad_w.shape[1:]
    colours = axis_orders(bits, rows)
    anywhere = pl.BlockSpec(memory_space=pl.ANY)
    onchip = pl.BlockSpec(memory_space=pltpu.VMEM)
    sems = pltpu.SemaphoreType.DMA
    levels = [
        pltpu.VMEM((2,) * (bits - 1 - step) + (size, cols), BF)
        for _, size, _ in colours
        for step in range(bits)
    ]
    return pl.pallas_call(
        functools.partial(tail_kernel, devices=devices, members=members),
        in_specs=[anywhere, onchip, onchip],
        out_specs=[anywhere, onchip, onchip],
        out_shape=[
            jax.ShapeDtypeStruct(grad_rows.shape, BF),
            jax.ShapeDtypeStruct((rows, cols), F32),
            jax.ShapeDtypeStruct(small.shape, F32),
        ],
        scratch_shapes=[pltpu.VMEM((stripe, features), BF)] + levels + levels + [
            pltpu.VMEM((bits,) + small.shape, F32), pltpu.VMEM((bits,) + small.shape, F32),
            sems((devices,)), sems((devices,)), sems((len(colours), bits)), sems((len(colours), bits)),
            sems((bits,)), sems((bits,)), sems((1,)),
        ],
        compiler_params=pltpu.CompilerParams(
            collective_id=1, has_side_effects=True, vmem_limit_bytes=VMEM_BYTES
        ),
        name="tail",
    )(grad_rows, grad_w.reshape((2,) * bits + (rows, cols)), small)


def body(
    tokens, out_grad, lengths, order, w_qkv, b_qkv, w_out, b_out, norm1_gain, norm1_bias,
    w_up, b_up, w_down, b_down, norm2_gain, norm2_bias,
):
    dp_size = lax.axis_size("dp")
    tp_size = lax.axis_size("tensor")
    devices = dp_size * tp_size
    stored, stripe, features = tokens.shape
    slot = devices * stripe
    depth = w_qkv.shape[1]
    cols = w_qkv.shape[2]
    units = w_up.shape[1]

    def deal(rows_val):
        return lax.all_to_all(rows_val, AXES, split_axis=0, concat_axis=0, tiled=True)

    ffn_shard = jnp.concatenate([w_up, w_down.T], axis=0)
    ffn_all = lax.all_gather(ffn_shard, AXES, axis=0, tiled=True)
    ffn_w = merge_groups(ffn_all.reshape(dp_size, tp_size, 2 * depth, units), 2)
    attn_shard = jnp.concatenate([w_qkv.reshape(3 * depth, cols), w_out.T], axis=0)
    biases = jnp.concatenate([b_qkv.reshape(-1), b_up]).reshape(-1, LANES)
    rows, attn_all, biases, cos_table, sine_table, mask = head(
        tokens, attn_shard, biases, order, lengths, tp_size
    )
    rows = rows.reshape(slot, features)
    attn_w = merge_groups(attn_all.reshape(dp_size, tp_size, 4 * depth, cols), 4)
    biases = biases.reshape(tp_size, -1)
    b_qkv_all = biases[:, : 3 * cols].reshape(tp_size, 3, cols).transpose(1, 0, 2).reshape(3, features)
    b_up_all = biases[:, 3 * cols :].reshape(1, tp_size * units)
    rows, out_grad = lax.optimization_barrier((rows, out_grad))
    cotangent = deal(out_grad).reshape(slot, features)
    none = jnp.zeros_like(b_out)
    vectors = jnp.stack(
        [b_out, norm1_gain, norm1_bias, b_down, norm2_gain, norm2_bias, none, none], axis=0
    )
    result, grad_rows, g_attn_w, g_ffn, packed = layer(
        rows, cotangent, mask, cos_table, sine_table, attn_w, ffn_w, b_qkv_all, b_up_all, vectors
    )
    mixed = deal(result.reshape(devices, stripe, features))
    laid = split_groups(g_ffn, 2, dp_size).reshape(devices * 2 * depth, units)
    ffn_sum = lax.psum_scatter(laid, AXES, scatter_dimension=0, tiled=True).astype(F32)
    laid = split_groups(g_attn_w, 4, dp_size).reshape(devices, 4 * depth, cols)
    packed = jnp.pad(packed, ((0, -packed.shape[0] % 8), (0, 0)))
    grad_tokens, attn_sum, summed = tail(
        grad_rows.reshape(devices, stripe, features), laid, packed, tp_size
    )
    return (
        mixed, grad_tokens, attn_sum[: 3 * depth].reshape(3, depth, cols), summed[:3],
        attn_sum[3 * depth :].T, summed[3], summed[4], summed[5], ffn_sum[:depth],
        summed[9:13].reshape(-1), ffn_sum[depth:].T, summed[6], summed[7], summed[8],
    )


def solution(mesh):
    rows = P(None, AXES, None)
    in_specs = (
        rows, rows, P(), P(), P(None, "dp", "tensor"), P(None, "tensor"), P("tensor", "dp"), P(),
        P(), P(), P("dp", "tensor"), P("tensor"), P("tensor", "dp"), P(), P(), P(),
    )
    out_specs = (
        rows, rows, P(None, "dp", "tensor"), P(), P("tensor", "dp"), P(), P(), P(),
        P("dp", "tensor"), P(), P("tensor", "dp"), P(), P(), P(),
    )
    return jax.shard_map(body, mesh=mesh, in_specs=in_specs, out_specs=out_specs, check_vma=False)
```
